32 devices in a mesh: tm: 16 (over z, y, x), space: 2 (over core).
Axes of the slice: x: 2, y: 2, z: 4, core: 2. Of those that a mesh axis runs over, the one named last changes fastest.
Arguments:
- initial: float32 [16, 32, 64, 128], P('tm', 'space'), may hold values from -6 to 6
- source: float32 [16, 32, 64, 128], P('tm', 'space'), may hold values from -6 to 6
- diffusion: float32 [32, 64, 128], P('space'), may hold values from 0.1 to 1
- advection: float32 [3, 32, 64, 128], P(None, 'space'), may hold values from 0.05 to 0.5
Outputs:
- smoothed: float32 [16, 32, 64, 128], P('tm', 'space')
- residual: float32 [16, 32, 64, 128], P('tm', 'space')
The draws below stay inside these ranges and needn't reach their ends.
All inputs are finite; a program needn't handle non-finite values.
Results may differ from the reference program's by a relative error of at most 0.00002.
Values sent between devices are 32-bit elements; how exact they have to be, the bound alone decides.
A program may use at most 64 MiB of HBM per device.

```python
import math
import jax
import jax.numpy as jnp

SWEEPS = 2
ITERS = 4
NX = 64
NY = 128
NT = 16
NZ = 32


def level_of(stream_key, dims, pieces, smallest, top_value):
    def one(position, shards_of):
        draws = jax.random.uniform(jax.random.fold_in(jax.random.fold_in(stream_key, 6), position), (shards_of,), jnp.float32, smallest / len(pieces), top_value / len(pieces))
        return jnp.repeat(jnp.exp(draws), dims[position] // shards_of).reshape((-1,) + (1,) * (len(dims) - position - 1))

    level = one(*pieces[0])
    for cut in pieces[1:]:
        level = level * one(*cut)
    return level


def normal_values(own_key, shape, deviation, most, shards=(), kind=jnp.bfloat16):
    drawn = jax.random.normal(own_key, shape, jnp.float32) * deviation
    if len(shards) > 0:
        drawn = level_of(own_key, shape, shards, -0.22, 0.18) * drawn
    return jnp.clip(drawn, min=-most, max=most).astype(kind)


def setup_inputs(seed: int = 0) -> dict:
    seeds = jax.random.split(jax.random.key(seed), 5)
    initial = normal_values(seeds[0], (NT, NZ, NX, NY), 1.0, 6.0, ((0, 16), (1, 2)), jnp.float32)
    source = normal_values(seeds[1], (NT, NZ, NX, NY), 1.0, 6.0, ((0, 16), (1, 2)), jnp.float32)
    diffusion = jnp.clip(jnp.exp(math.log(1.0) - 2.3025851 * jax.random.uniform(seeds[2], (NZ, NX, NY), jnp.float32) ** level_of(seeds[2], (NZ, NX, NY), ((0, 2),), -0.2, 0.2)), 0.1, 1.0)
    advection = jnp.clip(jnp.exp(math.log(0.5) - 2.3025851 * jax.random.uniform(seeds[3], (3, NZ, NX, NY), jnp.float32) ** level_of(seeds[3], (3, NZ, NX, NY), ((1, 2),), -0.2, 0.2)), 0.05, 0.5)
    return {"initial": initial, "source": source, "diffusion": diffusion, "advection": advection}


def off_terms(padded, spread, upwind):
    low_z = padded[..., :-2, 1:-1, 1:-1]
    high_z = padded[..., 2:, 1:-1, 1:-1]
    low_x = padded[..., 1:-1, :-2, 1:-1]
    high_x = padded[..., 1:-1, 2:, 1:-1]
    low_y = padded[..., 1:-1, 1:-1, :-2]
    high_y = padded[..., 1:-1, 1:-1, 2:]
    total = spread * (high_z + low_z + high_x + low_x + high_y + low_y)
    return total + upwind[0] * low_x + upwind[1] * low_y + upwind[2] * low_z


def main_diagonal(spread, upwind):
    return 1.0 + 6.0 * spread + (upwind[0] + upwind[1] + upwind[2])


def pad_space(field):
    return jnp.pad(field, ((0, 0), (1, 1), (1, 1), (1, 1)))


def reference(initial, source, diffusion, advection):
    diagonal = main_diagonal(diffusion, advection)
    smoothed = initial
    for sweep in range(SWEEPS):
        prior = jnp.roll(smoothed, 1, axis=0)
        forcing = prior + source
        current = smoothed
        for step in range(ITERS):
            current = (forcing + off_terms(pad_space(current), diffusion, advection)) / diagonal
        smoothed = current
    prior = jnp.roll(smoothed, 1, axis=0)
    applied = diagonal * smoothed - off_terms(pad_space(smoothed), diffusion, advection)
    residual = source + prior - applied
    return smoothed, residual
```

```python
import functools

import jax
import jax.numpy as jnp
from jax import lax
from jax.experimental import pallas as pl
from jax.experimental.pallas import tpu as pltpu
from jax.sharding import PartitionSpec as P

ITERS = 4
HALO = ITERS
STEP = 2
LAG = 3
VMEM_BYTES = 67043328
MESH = pl.DeviceIdType.MESH


def kernel(planes, steps, relayed, initial, source, diffusion, advection, s2, res,
           u, src, spread, upwind, low_z, high_z, low_x, high_x, low_y, high_y, inverse, diagonal,
           base, forced, y0, y1, y2, y3, v1, v2, v3, g, e, z, e_in, z_in, r, p3,
           load_sem, send_e, recv_e, send_z, recv_z, send_s, recv_s, send_f, hsend, hrecv):
    count = planes // STEP
    half = planes // 2
    time, side = lax.axis_index("tm"), lax.axis_index("space")
    odd = lax.rem(time, 2)
    partner = time + 1 - 2 * odd
    after, before = lax.rem(time + 1, steps), lax.rem(time + steps - 1, steps)
    beyond, behind = lax.rem(time + 2, steps), lax.rem(time + steps - 2, steps)
    other = 1 - side
    rows, lanes = u.shape[1], u.shape[2]

    def begin(lo, hi, who=side):
        return (1 - who) * (HALO + lo) + who * (HALO + planes - hi)

    def span(lo, hi, who=side):
        return pl.ds(begin(lo, hi, who), hi - lo if isinstance(lo, int) else STEP)

    def grid_span(lo, hi):
        return pl.ds(begin(lo, hi) - HALO, hi - lo)

    def part(k):
        return pl.ds(begin(STEP * k, STEP * k + STEP), STEP)

    barrier = pltpu.get_barrier_semaphore()
    for peer in ((partner, side), (behind, side), (before, side), (time, other)):
        pl.semaphore_signal(barrier, inc=1, device_id=peer, device_id_type=MESH)

    loads = []
    for n, (lo, hi) in enumerate(((0, half), (half, planes))):
        here, there = span(lo, hi), grid_span(lo, hi)
        loads.append([
            pltpu.make_async_copy(diffusion.at[there], spread.at[here], load_sem.at[n, 0]),
            pltpu.make_async_copy(advection.at[:, there], upwind.at[:, here], load_sem.at[n, 1]),
            pltpu.make_async_copy(initial.at[0, there], u.at[here], load_sem.at[n, 2]),
            pltpu.make_async_copy(source.at[0, there], src.at[here], load_sem.at[n, 3]),
        ])
    for group in loads:
        for load in group:
            load.start()

    edge = begin(-1, 0)
    for field in (u, y0, y1, y2, y3, v1, v2, v3, g, s2):
        field[edge] = jnp.zeros((rows, lanes), jnp.float32)

    def across(source_ref, target_ref, n):
        return pltpu.make_async_remote_copy(
            src_ref=source_ref, dst_ref=target_ref, send_sem=hsend.at[n], recv_sem=hrecv.at[n],
            device_id=(time, other), device_id_type=MESH)

    def rim(field, width, n):
        return across(field.at[span(planes - width, planes)],
                      field.at[span(planes, planes + width, other)], n)

    mine, theirs = grid_span(planes - HALO, planes), span(planes, planes + HALO, other)
    rims = [
        across(diffusion.at[mine], spread.at[theirs], 0),
        across(advection.at[:, mine], upwind.at[:, theirs], 1),
        across(initial.at[0, mine], u.at[theirs], 2),
        across(source.at[0, mine], src.at[theirs], 3),
    ]
    rim_g, rim_r, rim_s = rim(g, HALO, 4), rim(r, HALO - 1, 5), rim(s2, 1, 6)

    def swap(k):
        return pltpu.make_async_remote_copy(
            src_ref=e.at[part(k)], dst_ref=e_in.at[part(k)], send_sem=send_e.at[k], recv_sem=recv_e.at[k],
            device_id=(partner, side), device_id_type=MESH)

    def hand(k):
        return pltpu.make_async_remote_copy(
            src_ref=z.at[part(k)], dst_ref=z_in.at[part(k)], send_sem=send_z.at[k], recv_sem=recv_z.at[k],
            device_id=(beyond, side), device_id_type=MESH)

    def pass_on(m):
        detour = odd * jnp.where(m < relayed, 1, 0)
        return pltpu.make_async_remote_copy(
            src_ref=s2.at[part(m)], dst_ref=p3.at[detour, part(m)], send_sem=send_s.at[m],
            recv_sem=recv_s.at[detour, m],
            device_id=(jnp.where(detour == 1, beyond, after), side), device_id_type=MESH)

    def forward(m):
        return pltpu.make_async_remote_copy(
            src_ref=p3.at[1, part(m)], dst_ref=p3.at[0, part(m)], send_sem=send_f.at[m],
            recv_sem=recv_s.at[0, m], device_id=(before, side), device_id_type=MESH)

    def detoured(m):
        return pltpu.make_async_remote_copy(
            src_ref=s2.at[part(m)], dst_ref=p3.at[1, part(m)], send_sem=send_s.at[m],
            recv_sem=recv_s.at[1, m], device_id=(beyond, side), device_id_type=MESH)

    def arrival(m):
        return pltpu.make_async_remote_copy(
            src_ref=s2.at[part(m)], dst_ref=p3.at[0, part(m)], send_sem=send_s.at[m],
            recv_sem=recv_s.at[0, m], device_id=(after, side), device_id_type=MESH)

    def each(lo, hi, body):
        start = begin(lo, hi)
        for k in range(hi - lo):
            body(start + k)

    def pair(lo, body):
        start = begin(lo, lo + STEP)
        for k in range(STEP):
            body(start + k)

    row = lax.broadcasted_iota(jnp.int32, (rows, lanes), 0)
    lane = lax.broadcasted_iota(jnp.int32, (rows, lanes), 1)

    def coefficients(i):
        d = spread[i]
        ax, ay, az = upwind[0, i], upwind[1, i], upwind[2, i]
        main = 1.0 + 6.0 * d + (ax + ay + az)
        inv = 1.0 / main
        even = d * inv
        high_z[i] = even
        low_z[i] = (d + az) * inv
        high_x[i] = jnp.where(row == rows - 1, 0.0, even)
        low_x[i] = jnp.where(row == 0, 0.0, (d + ax) * inv)
        high_y[i] = jnp.where(lane == lanes - 1, 0.0, even)
        low_y[i] = jnp.where(lane == 0, 0.0, (d + ay) * inv)
        inverse[i] = inv
        diagonal[i] = main
        y0[i] = u[i] * inv
        base[i] = src[i] * inv

    def neighbours(v, i):
        here = v[i]
        total = low_z[i] * v[i - 1] + high_z[i] * v[i + 1]
        total += low_x[i] * pltpu.roll(here, 1, 0) + high_x[i] * pltpu.roll(here, rows - 1, 0)
        return total + (low_y[i] * pltpu.roll(here, 1, 1) + high_y[i] * pltpu.roll(here, lanes - 1, 1))

    powers, bases = [y0, y1, y2, y3], [u, v1, v2, v3]

    def lift(n):
        def one(i):
            y = neighbours(powers[n - 1], i)
            b = base[i] + neighbours(bases[n - 1], i)
            if n < ITERS:
                powers[n][i] = y
                bases[n][i] = b
            else:
                g[i] = b
                e[i] = b + diagonal[i] * y
                z[i] = (y0[i] + y1[i]) + (y2[i] + y3[i])
        return one

    def emit(k):
        swap(k).start()

        @pl.when(odd == 1)
        def _():
            hand(k).start()

    for load in loads[0]:
        load.wait()
    each(0, STEP + ITERS, coefficients)
    for n in range(1, ITERS + 1):
        each(0, STEP + ITERS - n, lift(n))
    pl.semaphore_wait(barrier, 4)
    emit(0)
    for copy in rims:
        copy.start()

    def local(k, carry):
        lo = STEP * k

        @pl.when(lo + ITERS == half)
        def _():
            for load in loads[1]:
                load.wait()

        @pl.when(lo + ITERS == planes)
        def _():
            for copy in rims:
                copy.wait_recv()

        pair(lo + ITERS, coefficients)
        for n in range(1, ITERS + 1):
            pair(lo + ITERS - n, lift(n))
        emit(k)
        return carry

    lax.fori_loop(1, count, local, 0)
    rim_g.start()

    def combine(k):
        @pl.when(odd == 0)
        def _():
            swap(k).wait_recv()

            def one(i):
                z[i] = z[i] + e_in[i]

            pair(STEP * k, one)
            hand(k).start()

    levels = [g, v1, v2, v3, s2]

    def force(i):
        forced[i] = (src[i] + r[i]) * inverse[i]

    def iterate(n):
        def one(i):
            levels[n][i] = forced[i] + neighbours(levels[n - 1], i)
        return one

    def gather(k):
        hand(k).wait_recv()

        @pl.when(odd == 1)
        def _():
            swap(k).wait_recv()

            def one(i):
                r[i] = z_in[i] + e_in[i]

            pair(STEP * k, one)

        @pl.when(odd == 0)
        def _():
            def one(i):
                r[i] = z_in[i]

            pair(STEP * k, one)

        pair(STEP * k, force)

    for k in range(LAG):
        combine(k)
    reached = [0] * (ITERS + 1)
    for k in range(2):
        combine(k + LAG)
        gather(k)
        for n in range(1, ITERS + 1):
            goal = max(STEP * (k + 1) - (n - 1), 0)
            each(reached[n], goal, iterate(n))
            reached[n] = goal
    rim_g.wait_recv()

    def sweep(k, carry):
        @pl.when(k + LAG < count)
        def _():
            combine(k + LAG)

        gather(k)
        for n in range(1, ITERS + 1):
            pair(STEP * k - (n - 1), iterate(n))
        pass_on(k - 2).start()
        return carry

    lax.fori_loop(2, count, sweep, 0)
    rim_r.start()
    rim_r.wait_recv()
    each(planes, planes + HALO - 1, force)
    for n in range(1, ITERS + 1):
        each(planes - (n - 1), planes + ITERS - n, iterate(n))
    rim_s.start()
    pass_on(count - 2).start()
    pass_on(count - 1).start()

    @pl.when(odd == 1)
    def _():
        for m in range(relayed):
            detoured(m).wait_recv()
            forward(m).start()

    rim_s.wait_recv()

    def partial(k, carry):
        def one(i):
            res[i] = src[i] - diagonal[i] * (s2[i] - neighbours(s2, i))

        pair(STEP * k, one)
        return carry

    lax.fori_loop(0, count, partial, 0)

    def settle(m, carry):
        arrival(m).wait_recv()

        def one(i):
            res[i] = res[i] + p3[0, i]

        pair(STEP * m, one)
        return carry

    lax.fori_loop(0, count, settle, 0)

    def drain(k, carry):
        swap(k).wait_send()
        hand(k).wait_send()
        arrival(k).wait_send()
        return carry

    lax.fori_loop(0, count, drain, 0)

    @pl.when(odd == 1)
    def _():
        for m in range(relayed):
            forward(m).wait_send()

    for copy in rims + [rim_g, rim_r, rim_s]:
        copy.wait_send()


def finish(planes, s2, res, smoothed, residual, sem):
    copies = [
        pltpu.make_async_copy(s2.at[pl.ds(HALO, planes)], smoothed.at[0], sem.at[0]),
        pltpu.make_async_copy(res.at[pl.ds(HALO, planes)], residual.at[0], sem.at[1]),
    ]
    for copy in copies:
        copy.start()
    for copy in copies:
        copy.wait()


def body(steps, sides, initial, source, diffusion, advection):
    _, planes, rows, lanes = initial.shape
    assert sides == 2 and steps % 2 == 0 and planes % (2 * STEP) == 0
    count = planes // STEP
    relayed = 0
    shape = (planes + 2 * HALO, rows, lanes)
    wide = pltpu.VMEM(shape, jnp.float32)
    triple = pltpu.VMEM((3,) + shape, jnp.float32)
    double = pltpu.VMEM((2,) + shape, jnp.float32)
    dma = pltpu.SemaphoreType.DMA
    result = jax.ShapeDtypeStruct(initial.shape, jnp.float32)
    vmem = pl.BlockSpec(memory_space=pltpu.VMEM)
    hbm = pl.BlockSpec(memory_space=pltpu.HBM)
    grant = VMEM_BYTES - (2 * shape[0] + 4) * rows * lanes * 4
    held = pl.pallas_call(
        functools.partial(kernel, planes, steps, relayed),
        out_shape=(wide,) * 2,
        in_specs=[hbm] * 4,
        out_specs=(vmem,) * 2,
        scratch_shapes=[wide] * 3 + [triple] + [wide] * 23 + [double]
        + [dma((2, 4))] + [dma((count,))] * 5 + [dma((2, count)), dma((count,)), dma((7,)), dma((7,))],
        compiler_params=pltpu.CompilerParams(collective_id=0, has_side_effects=True, vmem_limit_bytes=grant),
        name="smooth",
    )(initial, source, diffusion, advection)
    return pl.pallas_call(
        functools.partial(finish, planes),
        out_shape=(result, result),
        in_specs=[vmem] * 2,
        out_specs=(hbm,) * 2,
        scratch_shapes=[dma((2,))],
        compiler_params=pltpu.CompilerParams(vmem_limit_bytes=8 << 20),
        name="finish",
    )(*held)


def solution(mesh):
    in_specs = (
        P("tm", "space", None, None),
        P("tm", "space", None, None),
        P("space", None, None),
        P(None, "space", None, None),
    )
    out_specs = (P("tm", "space", None, None), P("tm", "space", None, None))
    run = functools.partial(body, mesh.shape["tm"], mesh.shape["space"])
    return jax.shard_map(run, mesh=mesh, in_specs=in_specs, out_specs=out_specs, check_vma=False)
```

```python
import functools

import jax
import jax.numpy as jnp
from jax import lax
from jax.experimental import pallas as pl
from jax.experimental.pallas import tpu as pltpu
from jax.sharding import PartitionSpec as P

ITERS = 4
HALO = ITERS
STEP = 2
LAG = 3
VMEM_BYTES = 67043328
MESH = pl.DeviceIdType.MESH


def kernel(planes, steps, relayed, initial, source, diffusion, advection, s2, res,
           u, src, spread, upwind, low_z, high_z, low_x, high_x, low_y, high_y, inverse, diagonal,
           base, forced, y0, y1, y2, y3, v1, v2, v3, g, e, z, e_in, z_in, r, p3,
           load_sem, send_e, recv_e, send_z, recv_z, send_s, recv_s, send_f, hsend, hrecv):
    count = planes // STEP
    half = planes // 2
    time, side = lax.axis_index("tm"), lax.axis_index("space")
    odd = lax.rem(time, 2)
    partner = time + 1 - 2 * odd
    after, before = lax.rem(time + 1, steps), lax.rem(time + steps - 1, steps)
    beyond, behind = lax.rem(time + 2, steps), lax.rem(time + steps - 2, steps)
    other = 1 - side
    rows, lanes = u.shape[1], u.shape[2]

    def begin(lo, hi, who=side):
        return (1 - who) * (HALO + lo) + who * (HALO + planes - hi)

    def span(lo, hi, who=side):
        return pl.ds(begin(lo, hi, who), hi - lo if isinstance(lo, int) else STEP)

    def grid_span(lo, hi):
        return pl.ds(begin(lo, hi) - HALO, hi - lo)

    def part(k):
        return pl.ds(begin(STEP * k, STEP * k + STEP), STEP)

    barrier = pltpu.get_barrier_semaphore()
    for peer in ((partner, side), (behind, side), (before, side), (time, other)):
        pl.semaphore_signal(barrier, inc=1, device_id=peer, device_id_type=MESH)

    loads = []
    for n, (lo, hi) in enumerate(((0, half), (half, planes))):
        here, there = span(lo, hi), grid_span(lo, hi)
        loads.append([
            pltpu.make_async_copy(diffusion.at[there], spread.at[here], load_sem.at[n, 0]),
            pltpu.make_async_copy(advection.at[:, there], upwind.at[:, here], load_sem.at[n, 1]),
            pltpu.make_async_copy(initial.at[0, there], u.at[here], load_sem.at[n, 2]),
            pltpu.make_async_copy(source.at[0, there], src.at[here], load_sem.at[n, 3]),
        ])
    for group in loads:
        for load in group:
            load.start()

    edge = begin(-1, 0)
    for field in (u, y0, y1, y2, y3, v1, v2, v3, g, s2):
        field[edge] = jnp.zeros((rows, lanes), jnp.float32)

    def across(source_ref, target_ref, n):
        return pltpu.make_async_remote_copy(
            src_ref=source_ref, dst_ref=target_ref, send_sem=hsend.at[n], recv_sem=hrecv.at[n],
            device_id=(time, other), device_id_type=MESH)

    def rim(field, width, n):
        return across(field.at[span(planes - width, planes)],
                      field.at[span(planes, planes + width, other)], n)

    mine, theirs = grid_span(planes - HALO, planes), span(planes, planes + HALO, other)
    rims = [
        across(diffusion.at[mine], spread.at[theirs], 0),
        across(advection.at[:, mine], upwind.at[:, theirs], 1),
        across(initial.at[0, mine], u.at[theirs], 2),
        across(source.at[0, mine], src.at[theirs], 3),
    ]
    rim_g, rim_r, rim_s = rim(g, HALO, 4), rim(r, HALO - 1, 5), rim(s2, 1, 6)

    def swap(k):
        return pltpu.make_async_remote_copy(
            src_ref=e.at[part(k)], dst_ref=e_in.at[part(k)], send_sem=send_e.at[k], recv_sem=recv_e.at[k],
            device_id=(partner, side), device_id_type=MESH)

    def hand(k):
        return pltpu.make_async_remote_copy(
            src_ref=z.at[part(k)], dst_ref=z_in.at[part(k)], send_sem=send_z.at[k], recv_sem=recv_z.at[k],
            device_id=(beyond, side), device_id_type=MESH)

    def pass_on(m):
        detour = odd * jnp.where(m < relayed, 1, 0)
        return pltpu.make_async_remote_copy(
            src_ref=s2.at[part(m)], dst_ref=p3.at[detour, part(m)], send_sem=send_s.at[m],
            recv_sem=recv_s.at[detour, m],
            device_id=(jnp.where(detour == 1, beyond, after), side), device_id_type=MESH)

    def forward(m):
        return pltpu.make_async_remote_copy(
            src_ref=p3.at[1, part(m)], dst_ref=p3.at[0, part(m)], send_sem=send_f.at[m],
            recv_sem=recv_s.at[0, m], device_id=(before, side), device_id_type=MESH)

    def detoured(m):
        return pltpu.make_async_remote_copy(
            src_ref=s2.at[part(m)], dst_ref=p3.at[1, part(m)], send_sem=send_s.at[m],
            recv_sem=recv_s.at[1, m], device_id=(beyond, side), device_id_type=MESH)

    def arrival(m):
        return pltpu.make_async_remote_copy(
            src_ref=s2.at[part(m)], dst_ref=p3.at[0, part(m)], send_sem=send_s.at[m],
            recv_sem=recv_s.at[0, m], device_id=(after, side), device_id_type=MESH)

    def each(lo, hi, body):
        start = begin(lo, hi)
        for k in range(hi - lo):
            body(start + k)

    def pair(lo, body):
        start = begin(lo, lo + STEP)
        for k in range(STEP):
            body(start + k)

    row = lax.broadcasted_iota(jnp.int32, (rows, lanes), 0)
    lane = lax.broadcasted_iota(jnp.int32, (rows, lanes), 1)

    def coefficients(i):
        d = spread[i]
        ax, ay, az = upwind[0, i], upwind[1, i], upwind[2, i]
        main = 1.0 + 6.0 * d + (ax + ay + az)
        inv = 1.0 / main
        even = d * inv
        high_z[i] = even
        low_z[i] = (d + az) * inv
        high_x[i] = jnp.where(row == rows - 1, 0.0, even)
        low_x[i] = jnp.where(row == 0, 0.0, (d + ax) * inv)
        high_y[i] = jnp.where(lane == lanes - 1, 0.0, even)
        low_y[i] = jnp.where(lane == 0, 0.0, (d + ay) * inv)
        inverse[i] = inv
        diagonal[i] = main
        y0[i] = u[i] * inv
        base[i] = src[i] * inv

    def neighbours(v, i):
        here = v[i]
        total = low_z[i] * v[i - 1] + high_z[i] * v[i + 1]
        total += low_x[i] * pltpu.roll(here, 1, 0) + high_x[i] * pltpu.roll(here, rows - 1, 0)
        return total + (low_y[i] * pltpu.roll(here, 1, 1) + high_y[i] * pltpu.roll(here, lanes - 1, 1))

    powers, bases = [y0, y1, y2, y3], [u, v1, v2, v3]

    def lift(n):
        def one(i):
            y = neighbours(powers[n - 1], i)
            b = base[i] + neighbours(bases[n - 1], i)
            if n < ITERS:
                powers[n][i] = y
                bases[n][i] = b
            else:
                g[i] = b
                e[i] = b + diagonal[i] * y
                z[i] = (y0[i] + y1[i]) + (y2[i] + y3[i])
        return one

    def emit(k):
        swap(k).start()

        @pl.when(jnp.logical_and(odd == 1, k < relayed + 2))
        def _():
            hand(k).start()

    for load in loads[0]:
        load.wait()
    each(0, STEP + ITERS, coefficients)
    for n in range(1, ITERS + 1):
        each(0, STEP + ITERS - n, lift(n))
    pl.semaphore_wait(barrier, 4)
    emit(0)
    for copy in rims:
        copy.start()

    def local(k, carry):
        lo = STEP * k

        @pl.when(lo + ITERS == half)
        def _():
            for load in loads[1]:
                load.wait()

        @pl.when(lo + ITERS == planes)
        def _():
            for copy in rims:
                copy.wait_recv()

        pair(lo + ITERS, coefficients)
        for n in range(1, ITERS + 1):
            pair(lo + ITERS - n, lift(n))
        emit(k)
        return carry

    lax.fori_loop(1, count, local, 0)
    rim_g.start()

    def combine(k):
        @pl.when(odd == 0)
        def _():
            swap(k).wait_recv()

            def one(i):
                z[i] = z[i] + e_in[i]

            pair(STEP * k, one)
            hand(k).start()

    levels = [g, v1, v2, v3, s2]

    def force(i):
        forced[i] = (src[i] + r[i]) * inverse[i]

    def iterate(n):
        def one(i):
            levels[n][i] = forced[i] + neighbours(levels[n - 1], i)
        return one

    def gather(k):
        hand(k).wait_recv()

        @pl.when(odd == 1)
        def _():
            swap(k).wait_recv()

            def one(i):
                r[i] = z_in[i] + e_in[i]

            pair(STEP * k, one)

        @pl.when(odd == 0)
        def _():
            def one(i):
                r[i] = z_in[i]

            pair(STEP * k, one)

        pair(STEP * k, force)

    for k in range(LAG):
        combine(k)
    reached = [0] * (ITERS + 1)
    for k in range(2):
        combine(k + LAG)
        gather(k)
        for n in range(1, ITERS + 1):
            goal = max(STEP * (k + 1) - (n - 1), 0)
            each(reached[n], goal, iterate(n))
            reached[n] = goal
    rim_g.wait_recv()

    def sweep(k, carry):
        @pl.when(k + LAG < count)
        def _():
            combine(k + LAG)

        gather(k)
        for n in range(1, ITERS + 1):
            pair(STEP * k - (n - 1), iterate(n))
        pass_on(k - 2).start()

        @pl.when(jnp.logical_and(odd == 1, k == relayed + 1))
        def _():
            for m in range(relayed + 2, count):
                hand(m).start()
            for m in range(relayed):
                detoured(m).wait_recv()
                forward(m).start()

        return carry

    lax.fori_loop(2, count, sweep, 0)
    rim_r.start()
    rim_r.wait_recv()
    each(planes, planes + HALO - 1, force)
    for n in range(1, ITERS + 1):
        each(planes - (n - 1), planes + ITERS - n, iterate(n))
    rim_s.start()
    pass_on(count - 2).start()
    pass_on(count - 1).start()

    rim_s.wait_recv()

    def partial(k, carry):
        def one(i):
            res[i] = src[i] - diagonal[i] * (s2[i] - neighbours(s2, i))

        pair(STEP * k, one)
        return carry

    lax.fori_loop(0, count, partial, 0)

    def settle(m, carry):
        arrival(m).wait_recv()

        def one(i):
            res[i] = res[i] + p3[0, i]

        pair(STEP * m, one)
        return carry

    lax.fori_loop(0, count, settle, 0)

    def drain(k, carry):
        swap(k).wait_send()
        hand(k).wait_send()
        arrival(k).wait_send()
        return carry

    lax.fori_loop(0, count, drain, 0)

    @pl.when(odd == 1)
    def _():
        for m in range(relayed):
            forward(m).wait_send()

    for copy in rims + [rim_g, rim_r, rim_s]:
        copy.wait_send()


def finish(planes, s2, res, smoothed, residual, sem):
    copies = [
        pltpu.make_async_copy(s2.at[pl.ds(HALO, planes)], smoothed.at[0], sem.at[0]),
        pltpu.make_async_copy(res.at[pl.ds(HALO, planes)], residual.at[0], sem.at[1]),
    ]
    for copy in copies:
        copy.start()
    for copy in copies:
        copy.wait()


def body(steps, sides, initial, source, diffusion, advection):
    _, planes, rows, lanes = initial.shape
    assert sides == 2 and steps % 2 == 0 and planes % (2 * STEP) == 0
    count = planes // STEP
    relayed = 3
    shape = (planes + 2 * HALO, rows, lanes)
    wide = pltpu.VMEM(shape, jnp.float32)
    triple = pltpu.VMEM((3,) + shape, jnp.float32)
    double = pltpu.VMEM((2,) + shape, jnp.float32)
    dma = pltpu.SemaphoreType.DMA
    result = jax.ShapeDtypeStruct(initial.shape, jnp.float32)
    vmem = pl.BlockSpec(memory_space=pltpu.VMEM)
    hbm = pl.BlockSpec(memory_space=pltpu.HBM)
    grant = VMEM_BYTES - (2 * shape[0] + 4) * rows * lanes * 4
    held = pl.pallas_call(
        functools.partial(kernel, planes, steps, relayed),
        out_shape=(wide,) * 2,
        in_specs=[hbm] * 4,
        out_specs=(vmem,) * 2,
        scratch_shapes=[wide] * 3 + [triple] + [wide] * 23 + [double]
        + [dma((2, 4))] + [dma((count,))] * 5 + [dma((2, count)), dma((count,)), dma((7,)), dma((7,))],
        compiler_params=pltpu.CompilerParams(collective_id=0, has_side_effects=True, vmem_limit_bytes=grant),
        name="smooth",
    )(initial, source, diffusion, advection)
    return pl.pallas_call(
        functools.partial(finish, planes),
        out_shape=(result, result),
        in_specs=[vmem] * 2,
        out_specs=(hbm,) * 2,
        scratch_shapes=[dma((2,))],
        compiler_params=pltpu.CompilerParams(vmem_limit_bytes=8 << 20),
        name="finish",
    )(*held)


def solution(mesh):
    in_specs = (
        P("tm", "space", None, None),
        P("tm", "space", None, None),
        P("space", None, None),
        P(None, "space", None, None),
    )
    out_specs = (P("tm", "space", None, None), P("tm", "space", None, None))
    run = functools.partial(body, mesh.shape["tm"], mesh.shape["space"])
    return jax.shard_map(run, mesh=mesh, in_specs=in_specs, out_specs=out_specs, check_vma=False)
```

```python
import functools

import jax
import jax.numpy as jnp
from jax import lax
from jax.experimental import pallas as pl
from jax.experimental.pallas import tpu as pltpu
from jax.sharding import PartitionSpec as P

ITERS = 4
HALO = ITERS
STEP = 2
LAG = 3
VMEM_BYTES = 67043328
MESH = pl.DeviceIdType.MESH
EXTRA = 1
REACH = [3, 3, 3, 3, 3]
EARLY = [5, 8, 5, 5, 8, 0]
ORDERS = [['', '', 'W5 W6 W7 F0 F1 F2', '', '', '', ''], ['', '', '', '', '', '', 'F1 F2'], ['', '', 'W5 W6 W7', '', 'F0', 'F1', 'F2'], ['', '', 'W5 W6 W7 F0 F1 F2', '', '', '', ''], ['', '', 'F0 F1 F2', '', '', '', ''], ['', '', '', '', '', 'G0', '']]


def kernel(planes, steps, relayed, initial, source, diffusion, advection, s2, res,
           u, src, spread, upwind, low_z, low_x, low_y, even, inverse, diagonal,
           base, forced, y0, y1, y2, y3, v1, v2, v3, g, e, z, e_in, z_in, r, p3,
           load_sem, send_e, recv_e, send_z, recv_z, send_s, recv_s, send_f, hsend, hrecv):
    count = planes // STEP
    half = planes // 2
    time, side = lax.axis_index("tm"), lax.axis_index("space")
    odd = lax.rem(time, 2)
    partner = time + 1 - 2 * odd
    after, before = lax.rem(time + 1, steps), lax.rem(time + steps - 1, steps)
    beyond, behind = lax.rem(time + 2, steps), lax.rem(time + steps - 2, steps)
    other = 1 - side
    rows, lanes = u.shape[1], u.shape[2]

    def begin(lo, hi, who=side):
        return (1 - who) * (HALO + lo) + who * (HALO + planes - hi)

    def span(lo, hi, who=side):
        return pl.ds(begin(lo, hi, who), hi - lo if isinstance(lo, int) else STEP)

    def grid_span(lo, hi):
        return pl.ds(begin(lo, hi) - HALO, hi - lo)

    def part(k):
        return pl.ds(begin(STEP * k, STEP * k + STEP), STEP)

    zone = odd - 1 + sum(
        jnp.where(time == at, n, 0) for n, at in ((1, 1), (2, 3), (3, steps - 3), (4, steps - 1), (6, steps - 4)))
    reach = sum(jnp.where(zone == n, REACH[n], 0) for n in range(len(REACH)))
    lag = LAG + jnp.where(time == 0, LAG, 0)
    early = sum(jnp.where(zone == n, EARLY[n], 0) for n in range(len(EARLY)))

    barrier = pltpu.get_barrier_semaphore()
    for peer in ((partner, side), (behind, side), (before, side), (time, other)):
        pl.semaphore_signal(barrier, inc=1, device_id=peer, device_id_type=MESH)
    if EXTRA:
        for here, there in ((0, steps - 4), (steps - 4, steps - 1)):
            @pl.when(time == here)
            def _():
                pl.semaphore_signal(barrier, inc=1, device_id=(there, side), device_id_type=MESH)

    loads = []
    for n, (lo, hi) in enumerate(((0, half), (half, planes))):
        here, there = span(lo, hi), grid_span(lo, hi)
        loads.append([
            pltpu.make_async_copy(diffusion.at[there], spread.at[here], load_sem.at[n, 0]),
            pltpu.make_async_copy(advection.at[:, there], upwind.at[:, here], load_sem.at[n, 1]),
            pltpu.make_async_copy(initial.at[0, there], u.at[here], load_sem.at[n, 2]),
            pltpu.make_async_copy(source.at[0, there], src.at[here], load_sem.at[n, 3]),
        ])
    for group in loads:
        for load in group:
            load.start()

    edge = begin(-1, 0)
    for field in (u, y0, y1, y2, y3, v1, v2, v3, g, s2):
        field[edge] = jnp.zeros((rows, lanes), jnp.float32)

    def across(source_ref, target_ref, n):
        return pltpu.make_async_remote_copy(
            src_ref=source_ref, dst_ref=target_ref, send_sem=hsend.at[n], recv_sem=hrecv.at[n],
            device_id=(time, other), device_id_type=MESH)

    def rim(field, width, n):
        return across(field.at[span(planes - width, planes)],
                      field.at[span(planes, planes + width, other)], n)

    mine, theirs = grid_span(planes - HALO, planes), span(planes, planes + HALO, other)
    rims = [
        across(diffusion.at[mine], spread.at[theirs], 0),
        across(advection.at[:, mine], upwind.at[:, theirs], 1),
        across(initial.at[0, mine], u.at[theirs], 2),
        across(source.at[0, mine], src.at[theirs], 3),
    ]
    rim_g, rim_r, rim_s = rim(g, HALO, 4), rim(r, HALO - 1, 5), rim(s2, 1, 6)

    def swap(k):
        return pltpu.make_async_remote_copy(
            src_ref=e.at[part(k)], dst_ref=e_in.at[part(k)], send_sem=send_e.at[k], recv_sem=recv_e.at[k],
            device_id=(partner, side), device_id_type=MESH)

    def hand(k):
        return pltpu.make_async_remote_copy(
            src_ref=z.at[part(k)], dst_ref=z_in.at[part(k)], send_sem=send_z.at[k], recv_sem=recv_z.at[k],
            device_id=(beyond, side), device_id_type=MESH)

    def pass_on(m):
        detour = odd * jnp.where(m < reach, 1, 0)
        slot = detour * (1 + jnp.where(jnp.logical_and(zone == 4, m < EXTRA), 1, 0))
        to = jnp.where(slot == 0, after, jnp.where(slot == 1, beyond, steps - 4))
        return pltpu.make_async_remote_copy(
            src_ref=s2.at[part(m)], dst_ref=p3.at[slot, part(m)], send_sem=send_s.at[m],
            recv_sem=recv_s.at[slot, m], device_id=(to, side), device_id_type=MESH)

    def forward(slot, m):
        to = before if slot == 1 else 0
        return pltpu.make_async_remote_copy(
            src_ref=p3.at[slot, part(m)], dst_ref=p3.at[0, part(m)], send_sem=send_f.at[slot - 1, m],
            recv_sem=recv_s.at[0, m], device_id=(to, side), device_id_type=MESH)

    def detoured(slot, m):
        return pltpu.make_async_remote_copy(
            src_ref=s2.at[part(m)], dst_ref=p3.at[slot, part(m)], send_sem=send_s.at[m],
            recv_sem=recv_s.at[slot, m], device_id=(beyond, side), device_id_type=MESH)

    def arrival(m):
        return pltpu.make_async_remote_copy(
            src_ref=s2.at[part(m)], dst_ref=p3.at[0, part(m)], send_sem=send_s.at[m],
            recv_sem=recv_s.at[0, m], device_id=(after, side), device_id_type=MESH)

    def each(lo, hi, body):
        start = begin(lo, hi)
        for k in range(hi - lo):
            body(start + k)

    def pair(lo, body):
        start = begin(lo, lo + STEP)
        for k in range(STEP):
            body(start + k)

    row = lax.broadcasted_iota(jnp.int32, (rows, lanes), 0)
    lane = lax.broadcasted_iota(jnp.int32, (rows, lanes), 1)
    last_row = lax.broadcasted_iota(jnp.int32, (8, lanes), 0) == 7
    last_lane = lane == lanes - 1
    unit = 1 + jnp.minimum(time, 0)

    def coefficients(i):
        d = spread[i]
        ax, ay, az = upwind[0, i], upwind[1, i], upwind[2, i]
        main = 1.0 + 6.0 * d + (ax + ay + az)
        inv = 1.0 / main
        even[i] = d * inv
        low_z[i] = (d + az) * inv
        low_x[i] = jnp.where(row == 0, 0.0, (d + ax) * inv)
        low_y[i] = jnp.where(lane == 0, 0.0, (d + ay) * inv)
        inverse[i] = inv
        diagonal[i] = main
        y0[i] = u[i] * inv
        base[i] = src[i] * inv

    def neighbours(v, i):
        flat = v.reshape(v.shape[0] * rows, lanes)
        here = v[i]
        below = flat[pl.ds(i * rows + unit, rows), :]
        cut = rows - 8
        below = jnp.concatenate([below[:cut], jnp.where(last_row, 0.0, below[cut:])], axis=0)
        right = jnp.where(last_lane, 0.0, pltpu.roll(here, lanes - 1, 1))
        total = even[i] * ((v[i + 1] + below) + right)
        total += low_z[i] * v[i - 1] + low_x[i] * flat[pl.ds(i * rows - unit, rows), :]
        return total + low_y[i] * pltpu.roll(here, 1, 1)

    powers, bases = [y0, y1, y2, y3], [u, v1, v2, v3]

    def lift(n):
        def one(i):
            y = neighbours(powers[n - 1], i)
            b = base[i] + neighbours(bases[n - 1], i)
            if n < ITERS:
                powers[n][i] = y
                bases[n][i] = b
            else:
                g[i] = b
                e[i] = b + diagonal[i] * y
                z[i] = (y0[i] + y1[i]) + (y2[i] + y3[i])
        return one

    def emit(k):
        swap(k).start()

        @pl.when(jnp.logical_and(odd == 1, k < early))
        def _():
            hand(k).start()

    for load in loads[0]:
        load.wait()
    each(0, STEP + ITERS, coefficients)
    for n in range(1, ITERS + 1):
        each(0, STEP + ITERS - n, lift(n))
    pl.semaphore_wait(barrier, 4 + (jnp.where(zone >= 4, 1, 0) if EXTRA else 0))
    emit(0)
    for copy in rims:
        copy.start()

    def local(k, carry):
        lo = STEP * k

        @pl.when(lo + ITERS == half)
        def _():
            for load in loads[1]:
                load.wait()

        @pl.when(lo + ITERS == planes)
        def _():
            for copy in rims:
                copy.wait_recv()

        pair(lo + ITERS, coefficients)
        for n in range(1, ITERS + 1):
            pair(lo + ITERS - n, lift(n))
        emit(k)
        return carry

    lax.fori_loop(1, count, local, 0)
    rim_g.start()

    def combine(k):
        @pl.when(odd == 0)
        def _():
            swap(k).wait_recv()

            def one(i):
                z[i] = z[i] + e_in[i]

            pair(STEP * k, one)
            hand(k).start()

    levels = [g, v1, v2, v3, s2]

    def force(i):
        forced[i] = (src[i] + r[i]) * inverse[i]

    def iterate(n):
        def one(i):
            levels[n][i] = forced[i] + neighbours(levels[n - 1], i)
        return one

    def gather(k):
        hand(k).wait_recv()

        @pl.when(odd == 1)
        def _():
            swap(k).wait_recv()

            def one(i):
                r[i] = z_in[i] + e_in[i]

            pair(STEP * k, one)

        @pl.when(odd == 0)
        def _():
            def one(i):
                r[i] = z_in[i]

            pair(STEP * k, one)

        pair(STEP * k, force)

    def act(order):
        for what in order.split():
            n = int(what[1:])
            if what[0] == "W":
                hand(n).start()
            else:
                slot = 1 if what[0] == "F" else 2
                detoured(slot, n).wait_recv()
                forward(slot, n).start()

    for k in range(LAG):
        combine(k)
    for k in range(LAG, 2 * LAG):
        @pl.when(time == 0)
        def _():
            combine(k)
    reached = [0] * (ITERS + 1)
    for k in range(2):
        combine(k + lag)
        gather(k)
        for n in range(1, ITERS + 1):
            goal = max(STEP * (k + 1) - (n - 1), 0)
            each(reached[n], goal, iterate(n))
            reached[n] = goal
    rim_g.wait_recv()

    def sweep(k, carry):
        @pl.when(k + lag < count)
        def _():
            combine(k + lag)

        gather(k)
        for n in range(1, ITERS + 1):
            pair(STEP * k - (n - 1), iterate(n))
        pass_on(k - 2).start()

        for where in range(len(ORDERS)):
            for turn in range(2, count):
                if ORDERS[where][turn - 2]:
                    @pl.when(jnp.logical_and(zone == where, k == turn))
                    def _():
                        act(ORDERS[where][turn - 2])

        return carry

    lax.fori_loop(2, count, sweep, 0)
    rim_r.start()
    rim_r.wait_recv()
    each(planes, planes + HALO - 1, force)
    for n in range(1, ITERS + 1):
        each(planes - (n - 1), planes + ITERS - n, iterate(n))
    rim_s.start()
    pass_on(count - 2).start()
    pass_on(count - 1).start()

    for where in range(len(ORDERS)):
        if ORDERS[where][-1]:
            @pl.when(zone == where)
            def _():
                act(ORDERS[where][-1])

    rim_s.wait_recv()

    def partial(k, carry):
        def one(i):
            res[i] = src[i] - diagonal[i] * (s2[i] - neighbours(s2, i))

        pair(STEP * k, one)
        return carry

    lax.fori_loop(0, count, partial, 0)

    def settle(m, carry):
        arrival(m).wait_recv()

        def one(i):
            res[i] = res[i] + p3[0, i]

        pair(STEP * m, one)
        return carry

    lax.fori_loop(0, count, settle, 0)

    def drain(k, carry):
        swap(k).wait_send()
        hand(k).wait_send()
        arrival(k).wait_send()
        return carry

    lax.fori_loop(0, count, drain, 0)

    for where, order in enumerate(ORDERS):
        @pl.when(zone == where)
        def _():
            for what in " ".join(order).split():
                if what[0] != "W":
                    forward(1 if what[0] == "F" else 2, int(what[1:])).wait_send()

    for copy in rims + [rim_g, rim_r, rim_s]:
        copy.wait_send()


def finish(planes, s2, res, smoothed, residual, sem):
    copies = [
        pltpu.make_async_copy(s2.at[pl.ds(HALO, planes)], smoothed.at[0], sem.at[0]),
        pltpu.make_async_copy(res.at[pl.ds(HALO, planes)], residual.at[0], sem.at[1]),
    ]
    for copy in copies:
        copy.start()
    for copy in copies:
        copy.wait()


def body(steps, sides, initial, source, diffusion, advection):
    _, planes, rows, lanes = initial.shape
    assert sides == 2 and steps % 2 == 0 and planes % (2 * STEP) == 0
    count = planes // STEP
    relayed = 3
    shape = (planes + 2 * HALO, rows, lanes)
    wide = pltpu.VMEM(shape, jnp.float32)
    triple = pltpu.VMEM((3,) + shape, jnp.float32)
    slots = pltpu.VMEM((3,) + shape, jnp.float32)
    dma = pltpu.SemaphoreType.DMA
    result = jax.ShapeDtypeStruct(initial.shape, jnp.float32)
    vmem = pl.BlockSpec(memory_space=pltpu.VMEM)
    hbm = pl.BlockSpec(memory_space=pltpu.HBM)
    grant = VMEM_BYTES - (2 * shape[0] + 4) * rows * lanes * 4
    held = pl.pallas_call(
        functools.partial(kernel, planes, steps, relayed),
        out_shape=(wide,) * 2,
        in_specs=[hbm] * 4,
        out_specs=(vmem,) * 2,
        scratch_shapes=[wide] * 3 + [triple] + [wide] * 21 + [slots]
        + [dma((2, 4))] + [dma((count,))] * 5 + [dma((3, count)), dma((2, count)), dma((7,)), dma((7,))],
        compiler_params=pltpu.CompilerParams(collective_id=0, has_side_effects=True, vmem_limit_bytes=grant),
        name="smooth",
    )(initial, source, diffusion, advection)
    return pl.pallas_call(
        functools.partial(finish, planes),
        out_shape=(result, result),
        in_specs=[vmem] * 2,
        out_specs=(hbm,) * 2,
        scratch_shapes=[dma((2,))],
        compiler_params=pltpu.CompilerParams(vmem_limit_bytes=8 << 20),
        name="finish",
    )(*held)


def solution(mesh):
    in_specs = (
        P("tm", "space", None, None),
        P("tm", "space", None, None),
        P("space", None, None),
        P(None, "space", None, None),
    )
    out_specs = (P("tm", "space", None, None), P("tm", "space", None, None))
    run = functools.partial(body, mesh.shape["tm"], mesh.shape["space"])
    return jax.shard_map(run, mesh=mesh, in_specs=in_specs, out_specs=out_specs, check_vma=False)
```

```python
import functools

import jax
import jax.numpy as jnp
from jax import lax
from jax.experimental import pallas as pl
from jax.experimental.pallas import tpu as pltpu
from jax.sharding import PartitionSpec as P

ITERS = 4
HALO = ITERS
STEP = 2
LAG = 3
VMEM_BYTES = 67043328
MESH = pl.DeviceIdType.MESH
EXTRA = 1
REACH = [3, 3, 3, 3, 4]
EARLY = [5, 8, 5, 5, 8, 0]
ORDERS = [
    [[], [], ["W5", "W6", "W7", "F0", "F1", "F2"], [], [], [], []],
    [[], [], [], [], [], [], ["F1", "F2", "F3"]],
    [[], [], ["W5", "W6", "W7"], [], ["F0"], ["F1"], ["F2"]],
    [[], [], ["W5", "W6", "W7", "F0", "F1", "F2"], [], [], [], []],
    [[], [], ["F0", "F1", "F2"], [], [], [], []],
    [[], [], [], [], [], ["G0"], []],
]


def kernel(planes, steps, initial, source, diffusion, advection, s2, res,
           u, src, spread, upwind, low_z, low_x, low_y, even, inverse, diagonal,
           base, forced, y0, y1, y2, y3, v1, v2, v3, g, e, z, e_in, z_in, r, p3,
           load_sem, sent, recv_e, recv_z, recv_s, hrecv):
    count = planes // STEP
    half = planes // 2
    time, side = lax.axis_index("tm"), lax.axis_index("space")
    odd = lax.rem(time, 2)
    partner = time + 1 - 2 * odd
    after, before = lax.rem(time + 1, steps), lax.rem(time + steps - 1, steps)
    beyond, behind = lax.rem(time + 2, steps), lax.rem(time + steps - 2, steps)
    other = 1 - side
    rows, lanes = u.shape[1], u.shape[2]

    def begin(lo, hi, who=side):
        return (1 - who) * (HALO + lo) + who * (HALO + planes - hi)

    def span(lo, hi, who=side):
        return pl.ds(begin(lo, hi, who), hi - lo if isinstance(lo, int) else STEP)

    def grid_span(lo, hi):
        return pl.ds(begin(lo, hi) - HALO, hi - lo)

    def part(k):
        return pl.ds(begin(STEP * k, STEP * k + STEP), STEP)

    zone = odd - 1 + sum(
        jnp.where(time == at, n, 0) for n, at in ((1, 1), (2, 3), (3, steps - 3), (4, steps - 1), (6, steps - 4)))
    reach = sum(jnp.where(zone == n, REACH[n], 0) for n in range(len(REACH)))
    lag = LAG + jnp.where(time == 0, LAG, 0)
    early = sum(jnp.where(zone == n, EARLY[n], 0) for n in range(len(EARLY)))

    barrier = pltpu.get_barrier_semaphore()
    for peer in ((partner, side), (behind, side), (before, side), (time, other)):
        pl.semaphore_signal(barrier, inc=1, device_id=peer, device_id_type=MESH)
    if EXTRA:
        for here, there in ((0, steps - 4), (steps - 4, steps - 1)):
            @pl.when(time == here)
            def _():
                pl.semaphore_signal(barrier, inc=1, device_id=(there, side), device_id_type=MESH)

    loads = []
    for n, (lo, hi) in enumerate(((0, half), (half, planes))):
        here, there = span(lo, hi), grid_span(lo, hi)
        loads.append([
            pltpu.make_async_copy(diffusion.at[there], spread.at[here], load_sem.at[n]),
            pltpu.make_async_copy(advection.at[:, there], upwind.at[:, here], load_sem.at[n]),
            pltpu.make_async_copy(initial.at[0, there], u.at[here], load_sem.at[n]),
            pltpu.make_async_copy(source.at[0, there], src.at[here], load_sem.at[n]),
        ])
    for group in loads:
        for load in group:
            load.start()

    edge = begin(-1, 0)
    for field in (u, y0, y1, y2, y3, v1, v2, v3, g, s2):
        field[edge] = jnp.zeros((rows, lanes), jnp.float32)

    def across(source_ref, target_ref, n):
        return pltpu.make_async_remote_copy(
            src_ref=source_ref, dst_ref=target_ref, send_sem=sent.at[1], recv_sem=hrecv.at[n],
            device_id=(time, other), device_id_type=MESH)

    def rim(field, width, n):
        return across(field.at[span(planes - width, planes)],
                      field.at[span(planes, planes + width, other)], n)

    mine, theirs = grid_span(planes - HALO, planes), span(planes, planes + HALO, other)
    rims = [
        across(diffusion.at[mine], spread.at[theirs], 0),
        across(advection.at[:, mine], upwind.at[:, theirs], 0),
        across(initial.at[0, mine], u.at[theirs], 0),
        across(source.at[0, mine], src.at[theirs], 0),
    ]
    rim_g, rim_r, rim_s = rim(g, HALO, 1), rim(r, HALO - 1, 2), rim(s2, 1, 3)

    def swap(k):
        return pltpu.make_async_remote_copy(
            src_ref=e.at[part(k)], dst_ref=e_in.at[part(k)], send_sem=sent.at[0], recv_sem=recv_e.at[k],
            device_id=(partner, side), device_id_type=MESH)

    def hand(k):
        return pltpu.make_async_remote_copy(
            src_ref=z.at[part(k)], dst_ref=z_in.at[part(k)], send_sem=sent.at[0], recv_sem=recv_z.at[k],
            device_id=(beyond, side), device_id_type=MESH)

    depth = planes + 2 * HALO

    def place(slot, m):
        return p3.at[pl.ds(slot * depth + begin(STEP * m, STEP * m + STEP), STEP)]

    def landed(slot, m):
        return recv_s.at[slot * count - jnp.where(slot == 2, count - max(REACH), 0) + m]

    def pass_on(m):
        detour = odd * jnp.where(m < reach, 1, 0)
        slot = detour * (1 + jnp.where(jnp.logical_and(zone == 4, m < EXTRA), 1, 0))
        to = jnp.where(slot == 0, after, jnp.where(slot == 1, beyond, steps - 4))
        return pltpu.make_async_remote_copy(
            src_ref=s2.at[part(m)], dst_ref=place(slot, m), send_sem=sent.at[0],
            recv_sem=landed(slot, m), device_id=(to, side), device_id_type=MESH)

    def forward(slot, m):
        to = before if slot == 1 else 0
        return pltpu.make_async_remote_copy(
            src_ref=place(slot, m), dst_ref=place(0, m), send_sem=sent.at[2],
            recv_sem=landed(0, m), device_id=(to, side), device_id_type=MESH)

    def arrival(slot, m):
        return pltpu.make_async_remote_copy(
            src_ref=s2.at[part(m)], dst_ref=place(slot, m), send_sem=sent.at[0],
            recv_sem=landed(slot, m), device_id=(after, side), device_id_type=MESH)

    def loaded(n, amount):
        return pltpu.make_async_copy(p3.at[pl.ds(0, amount)], p3.at[pl.ds(0, amount)], load_sem.at[n])

    def total(n, amount):
        return pltpu.make_async_remote_copy(
            src_ref=p3.at[pl.ds(0, amount)], dst_ref=p3.at[pl.ds(0, amount)], send_sem=sent.at[n],
            recv_sem=hrecv.at[0], device_id=(time, other), device_id_type=MESH)

    def each(lo, hi, body):
        start = begin(lo, hi)
        for k in range(hi - lo):
            body(start + k)

    def pair(lo, body):
        start = begin(lo, lo + STEP)
        for k in range(STEP):
            body(start + k)

    row = lax.broadcasted_iota(jnp.int32, (rows, lanes), 0)
    lane = lax.broadcasted_iota(jnp.int32, (rows, lanes), 1)
    last_row = lax.broadcasted_iota(jnp.int32, (8, lanes), 0) == 7
    last_lane = lane == lanes - 1
    unit = 1 + jnp.minimum(time, 0)

    def coefficients(i):
        d = spread[i]
        ax, ay, az = upwind[0, i], upwind[1, i], upwind[2, i]
        main = 1.0 + 6.0 * d + (ax + ay + az)
        inv = 1.0 / main
        even[i] = d * inv
        low_z[i] = (d + az) * inv
        low_x[i] = jnp.where(row == 0, 0.0, (d + ax) * inv)
        low_y[i] = jnp.where(lane == 0, 0.0, (d + ay) * inv)
        inverse[i] = inv
        diagonal[i] = main
        y0[i] = u[i] * inv
        base[i] = src[i] * inv

    def neighbours(v, i):
        flat = v.reshape(v.shape[0] * rows, lanes)
        here = v[i]
        below = flat[pl.ds(i * rows + unit, rows), :]
        cut = rows - 8
        below = jnp.concatenate([below[:cut], jnp.where(last_row, 0.0, below[cut:])], axis=0)
        right = jnp.where(last_lane, 0.0, pltpu.roll(here, lanes - 1, 1))
        total = even[i] * ((v[i + 1] + below) + right)
        total += low_z[i] * v[i - 1] + low_x[i] * flat[pl.ds(i * rows - unit, rows), :]
        return total + low_y[i] * pltpu.roll(here, 1, 1)

    powers, bases = [y0, y1, y2, y3], [u, v1, v2, v3]

    def lift(n, whole=True):
        def one(i):
            y = neighbours(powers[n - 1], i)
            b = base[i] + neighbours(bases[n - 1], i)
            if n < ITERS:
                powers[n][i] = y
                bases[n][i] = b
            else:
                g[i] = b
                e[i] = b + diagonal[i] * y
                if whole:
                    spread_sum(i)
        return one

    def raise_power(n):
        def one(i):
            powers[n][i] = neighbours(powers[n - 1], i)
        return one

    def raise_base(n):
        def one(i):
            bases[n][i] = base[i] + neighbours(bases[n - 1], i)
        return one

    def spread_sum(i):
        z[i] = (y0[i] + y1[i]) + (y2[i] + y3[i])

    def emit(k):
        swap(k).start()

        @pl.when(jnp.logical_and(odd == 1, k < early))
        def _():
            hand(k).start()

    loaded(0, 6 * half).wait()
    each(0, STEP + ITERS, coefficients)
    for n in range(1, ITERS):
        each(0, STEP + ITERS - n, raise_power(n))
    each(0, STEP, spread_sum)
    pl.semaphore_wait(barrier, 4 + (jnp.where(zone >= 4, 1, 0) if EXTRA else 0))

    @pl.when(odd == 1)
    def _():
        hand(0).start()

    for n in range(1, ITERS):
        each(0, STEP + ITERS - n, raise_base(n))
    each(0, STEP, lift(ITERS, False))
    swap(0).start()
    for copy in rims:
        copy.start()

    def local(k, carry):
        lo = STEP * k

        @pl.when(lo + ITERS == half)
        def _():
            loaded(1, 6 * (planes - half)).wait()

        @pl.when(lo + ITERS == planes)
        def _():
            total(1, 6 * HALO).wait_recv()

        pair(lo + ITERS, coefficients)
        for n in range(1, ITERS + 1):
            pair(lo + ITERS - n, lift(n))
        emit(k)
        return carry

    lax.fori_loop(1, count, local, 0)
    rim_g.start()

    def combine(k):
        @pl.when(odd == 0)
        def _():
            swap(k).wait_recv()

            def one(i):
                z[i] = z[i] + e_in[i]

            pair(STEP * k, one)
            hand(k).start()

    levels = [g, v1, v2, v3, s2]

    def force(i):
        forced[i] = (src[i] + r[i]) * inverse[i]

    def iterate(n):
        def one(i):
            levels[n][i] = forced[i] + neighbours(levels[n - 1], i)
        return one

    def gather(k):
        hand(k).wait_recv()

        @pl.when(odd == 1)
        def _():
            swap(k).wait_recv()

            def one(i):
                r[i] = z_in[i] + e_in[i]

            pair(STEP * k, one)

        @pl.when(odd == 0)
        def _():
            def one(i):
                r[i] = z_in[i]

            pair(STEP * k, one)

        pair(STEP * k, force)

    def act(order):
        for what in order:
            n = int(what[1:])
            if what[0] == "W":
                hand(n).start()
            else:
                slot = 1 if what[0] == "F" else 2
                arrival(slot, n).wait_recv()
                forward(slot, n).start()

    for k in range(LAG):
        combine(k)
    for k in range(LAG, 2 * LAG):
        @pl.when(time == 0)
        def _():
            combine(k)
    reached = [0] * (ITERS + 1)
    for k in range(2):
        combine(k + lag)
        gather(k)
        for n in range(1, ITERS + 1):
            goal = max(STEP * (k + 1) - (n - 1), 0)
            each(reached[n], goal, iterate(n))
            reached[n] = goal
    rim_g.wait_recv()

    def sweep(k, carry):
        @pl.when(k + lag < count)
        def _():
            combine(k + lag)

        gather(k)
        for n in range(1, ITERS + 1):
            pair(STEP * k - (n - 1), iterate(n))
        pass_on(k - 2).start()

        for where in range(len(ORDERS)):
            for turn in range(2, count):
                if ORDERS[where][turn - 2]:
                    @pl.when(jnp.logical_and(zone == where, k == turn))
                    def _():
                        act(ORDERS[where][turn - 2])

        return carry

    lax.fori_loop(2, count, sweep, 0)
    rim_r.start()
    rim_r.wait_recv()
    each(planes, planes + HALO - 1, force)
    for n in range(1, ITERS + 1):
        each(planes - (n - 1), planes + ITERS - n, iterate(n))
    rim_s.start()

    def close():
        pass_on(count - 2).start()
        pass_on(count - 1).start()

    @pl.when(zone != 1)
    def _():
        close()

    for where in range(len(ORDERS)):
        if ORDERS[where][-1]:
            @pl.when(zone == where)
            def _():
                act(ORDERS[where][-1])

    @pl.when(zone == 1)
    def _():
        close()

    rim_s.wait_recv()

    def partial(k, carry):
        def one(i):
            res[i] = src[i] - diagonal[i] * (s2[i] - neighbours(s2, i))

        pair(STEP * k, one)
        return carry

    lax.fori_loop(0, count, partial, 0)

    def settle(m, carry):
        arrival(0, m).wait_recv()

        def one(i):
            res[i] = res[i] + p3[i]

        pair(STEP * m, one)
        return carry

    lax.fori_loop(0, count, settle, 0)

    total(0, 3 * planes).wait_send()
    total(1, 8 * HALO).wait_send()
    for where, order in enumerate(ORDERS):
        passed = sum(what[0] != "W" for what in sum(order, []))
        if passed:
            @pl.when(zone == where)
            def _():
                total(2, STEP * passed).wait_send()


def finish(planes, s2, res, smoothed, residual, sem):
    copies = [
        pltpu.make_async_copy(s2.at[pl.ds(HALO, planes)], smoothed.at[0], sem.at[0]),
        pltpu.make_async_copy(res.at[pl.ds(HALO, planes)], residual.at[0], sem.at[1]),
    ]
    for copy in copies:
        copy.start()
    for copy in copies:
        copy.wait()


def body(steps, sides, initial, source, diffusion, advection):
    _, planes, rows, lanes = initial.shape
    assert sides == 2 and steps % 2 == 0 and planes % (2 * STEP) == 0
    count = planes // STEP
    shape = (planes + 2 * HALO, rows, lanes)
    wide = pltpu.VMEM(shape, jnp.float32)
    triple = pltpu.VMEM((3,) + shape, jnp.float32)
    slots = pltpu.VMEM((3 * shape[0],) + shape[1:], jnp.float32)
    dma = pltpu.SemaphoreType.DMA
    result = jax.ShapeDtypeStruct(initial.shape, jnp.float32)
    vmem = pl.BlockSpec(memory_space=pltpu.VMEM)
    hbm = pl.BlockSpec(memory_space=pltpu.HBM)
    grant = VMEM_BYTES - (2 * shape[0] + 4) * rows * lanes * 4
    held = pl.pallas_call(
        functools.partial(kernel, planes, steps),
        out_shape=(wide,) * 2,
        in_specs=[hbm] * 4,
        out_specs=(vmem,) * 2,
        scratch_shapes=[wide] * 3 + [triple] + [wide] * 21 + [slots]
        + [dma((2,)), dma((3,))] + [dma((count,))] * 2
        + [dma((count + max(REACH) + EXTRA,)), dma((4,))],
        compiler_params=pltpu.CompilerParams(collective_id=0, has_side_effects=True, vmem_limit_bytes=grant),
        name="smooth",
    )(initial, source, diffusion, advection)
    return pl.pallas_call(
        functools.partial(finish, planes),
        out_shape=(result, result),
        in_specs=[vmem] * 2,
        out_specs=(hbm,) * 2,
        scratch_shapes=[dma((2,))],
        compiler_params=pltpu.CompilerParams(vmem_limit_bytes=8 << 20),
        name="finish",
    )(*held)


def solution(mesh):
    in_specs = (
        P("tm", "space", None, None),
        P("tm", "space", None, None),
        P("space", None, None),
        P(None, "space", None, None),
    )
    out_specs = (P("tm", "space", None, None), P("tm", "space", None, None))
    run = functools.partial(body, mesh.shape["tm"], mesh.shape["space"])
    return jax.shard_map(run, mesh=mesh, in_specs=in_specs, out_specs=out_specs, check_vma=False)
```

```python
import functools

import jax
import jax.numpy as jnp
from jax import lax
from jax.experimental import pallas as pl
from jax.experimental.pallas import tpu as pltpu
from jax.sharding import PartitionSpec as P

ITERS = 4
HALO = ITERS
STEP = 2
LAG = 3
VMEM_BYTES = 67043328
MESH = pl.DeviceIdType.MESH
REACH = [3, 3, 3, 2, 0]
ROUND = ((2, 0), (2, 1), (1, 0), (1, 0), (1, 0), (0, 0), (0, 0), (0, 0))
EARLY = [5, 8, 5, 5, 8]
ORDERS = [
    [[], [], ["W5", "W6", "W7", "F0", "F1", "F2"], [], [], [], []],
    [[], [], [], [], [], [], ["F2", "F3", "F4"]],
    [[], [], ["W5", "W6", "W7"], [], ["F0"], ["F1"], ["F2"]],
    [[], [], ["W5", "W6", "W7", "F0", "F1", "F2"], [], [], [], []],
    [[], [], ["F0", "F1"], [], [], [], []],
    [[], [], [], ["G0"], [], [], []],
    [[], [], [], ["G1"], [], [], []],
    [[], [], [], [], [], [], []],
]


def kernel(planes, steps, initial, source, diffusion, advection, s2, res,
           u, src, spread, upwind, low_z, low_x, low_y, even, inverse, diagonal,
           base, forced, y0, y1, y2, y3, v1, v2, v3, g, e, z, e_in, z_in, r, p3,
           load_sem, sent, recv_e, recv_z, recv_s, hrecv):
    count = planes // STEP
    half = planes // 2
    time, side = lax.axis_index("tm"), lax.axis_index("space")
    odd = lax.rem(time, 2)
    partner = time + 1 - 2 * odd
    after, before = lax.rem(time + 1, steps), lax.rem(time + steps - 1, steps)
    beyond, behind = lax.rem(time + 2, steps), lax.rem(time + steps - 2, steps)
    other = 1 - side
    rows, lanes = u.shape[1], u.shape[2]

    def begin(lo, hi, who=side):
        return (1 - who) * (HALO + lo) + who * (HALO + planes - hi)

    def span(lo, hi, who=side):
        return pl.ds(begin(lo, hi, who), hi - lo if isinstance(lo, int) else STEP)

    def grid_span(lo, hi):
        return pl.ds(begin(lo, hi) - HALO, hi - lo)

    def part(k):
        return pl.ds(begin(STEP * k, STEP * k + STEP), STEP)

    zone = odd - 1 + sum(
        jnp.where(time == at, n, 0) for n, at in ((1, 1), (2, 3), (3, steps - 3), (4, steps - 1), (6, steps - 4), (7, steps - 2)))
    reach = sum(jnp.where(zone == n, REACH[n], 0) for n in range(len(REACH)))
    lag = LAG + jnp.where(time == 0, LAG, 0)
    early = sum(jnp.where(zone == n, EARLY[n], 0) for n in range(len(EARLY)))

    barrier = pltpu.get_barrier_semaphore()
    for peer in ((partner, side), (behind, side), (before, side), (time, other)):
        pl.semaphore_signal(barrier, inc=1, device_id=peer, device_id_type=MESH)
    guests = (steps - 4,)
    for guest in guests:
        for here, there in ((0, guest), (guest, steps - 1)):
            @pl.when(time == here)
            def _():
                pl.semaphore_signal(barrier, inc=1, device_id=(there, side), device_id_type=MESH)

    greeted = 4 + sum(jnp.where(zone == n, extra, 0) for n, extra in ((4, 1), (5, 1)))

    loads = []
    for n, (lo, hi) in enumerate(((0, half), (half, planes))):
        here, there = span(lo, hi), grid_span(lo, hi)
        loads.append([
            pltpu.make_async_copy(diffusion.at[there], spread.at[here], load_sem.at[n]),
            pltpu.make_async_copy(advection.at[:, there], upwind.at[:, here], load_sem.at[n]),
            pltpu.make_async_copy(initial.at[0, there], u.at[here], load_sem.at[n]),
            pltpu.make_async_copy(source.at[0, there], src.at[here], load_sem.at[n]),
        ])
    for group in loads:
        for load in group:
            load.start()

    edge = begin(-1, 0)
    for field in (u, y0, y1, y2, y3, v1, v2, v3, g, s2):
        field[edge] = jnp.zeros((rows, lanes), jnp.float32)

    def across(source_ref, target_ref, n):
        return pltpu.make_async_remote_copy(
            src_ref=source_ref, dst_ref=target_ref, send_sem=sent.at[1], recv_sem=hrecv.at[n],
            device_id=(time, other), device_id_type=MESH)

    def rim(field, width, n):
        return across(field.at[span(planes - width, planes)],
                      field.at[span(planes, planes + width, other)], n)

    mine, theirs = grid_span(planes - HALO, planes), span(planes, planes + HALO, other)
    rims = [
        across(diffusion.at[mine], spread.at[theirs], 0),
        across(advection.at[:, mine], upwind.at[:, theirs], 0),
        across(initial.at[0, mine], u.at[theirs], 0),
        across(source.at[0, mine], src.at[theirs], 0),
    ]
    rim_g, rim_r, rim_s = rim(g, HALO, 1), rim(r, HALO - 1, 2), rim(s2, 1, 3)

    def swap(k):
        return pltpu.make_async_remote_copy(
            src_ref=e.at[part(k)], dst_ref=e_in.at[part(k)], send_sem=sent.at[0], recv_sem=recv_e.at[k],
            device_id=(partner, side), device_id_type=MESH)

    def hand(k):
        return pltpu.make_async_remote_copy(
            src_ref=z.at[part(k)], dst_ref=z_in.at[part(k)], send_sem=sent.at[0], recv_sem=recv_z.at[k],
            device_id=(beyond, side), device_id_type=MESH)

    depth = planes + 2 * HALO

    def place(slot, m):
        return p3.at[pl.ds(slot * depth + begin(STEP * m, STEP * m + STEP), STEP)]

    def landed(slot, m):
        return recv_s.at[jnp.where(slot == 0, m, count + jnp.where(slot == 1, m % 4, 4 + m % 2))]

    def pass_on(m):
        near = jnp.where(m < reach, 1, 0)
        far = sum(jnp.where(m == n, slot, 0) for n, (slot, _) in enumerate(ROUND))
        slot = odd * jnp.where(zone == 4, far, near)
        host = sum(jnp.where(m == n, (steps - 4, steps - 2)[at], 0) for n, (slot_, at) in enumerate(ROUND) if slot_ == 2)
        to = jnp.where(slot == 0, after, jnp.where(slot == 1, beyond, host))
        return pltpu.make_async_remote_copy(
            src_ref=s2.at[part(m)], dst_ref=place(slot, m), send_sem=sent.at[0],
            recv_sem=landed(slot, m), device_id=(to, side), device_id_type=MESH)

    def forward(slot, m):
        to = before if slot == 1 else 0
        return pltpu.make_async_remote_copy(
            src_ref=place(slot, m), dst_ref=place(0, m), send_sem=sent.at[2],
            recv_sem=landed(0, m), device_id=(to, side), device_id_type=MESH)

    def arrival(slot, m):
        return pltpu.make_async_remote_copy(
            src_ref=s2.at[part(m)], dst_ref=place(slot, m), send_sem=sent.at[0],
            recv_sem=landed(slot, m), device_id=(after, side), device_id_type=MESH)

    def loaded(n, amount):
        return pltpu.make_async_copy(p3.at[pl.ds(0, amount)], p3.at[pl.ds(0, amount)], load_sem.at[n])

    def total(n, amount):
        return pltpu.make_async_remote_copy(
            src_ref=p3.at[pl.ds(0, amount)], dst_ref=p3.at[pl.ds(0, amount)], send_sem=sent.at[n],
            recv_sem=hrecv.at[0], device_id=(time, other), device_id_type=MESH)

    def each(lo, hi, body):
        start = begin(lo, hi)
        for k in range(hi - lo):
            body(start + k)

    def pair(lo, body):
        start = begin(lo, lo + STEP)
        for k in range(STEP):
            body(start + k)

    row = lax.broadcasted_iota(jnp.int32, (rows, lanes), 0)
    lane = lax.broadcasted_iota(jnp.int32, (rows, lanes), 1)
    last_row = lax.broadcasted_iota(jnp.int32, (8, lanes), 0) == 7
    last_lane = lane == lanes - 1
    unit = 1 + jnp.minimum(time, 0)

    def coefficients(i):
        d = spread[i]
        ax, ay, az = upwind[0, i], upwind[1, i], upwind[2, i]
        main = 1.0 + 6.0 * d + (ax + ay + az)
        inv = 1.0 / main
        even[i] = d * inv
        low_z[i] = (d + az) * inv
        low_x[i] = jnp.where(row == 0, 0.0, (d + ax) * inv)
        low_y[i] = jnp.where(lane == 0, 0.0, (d + ay) * inv)
        inverse[i] = inv
        diagonal[i] = main
        y0[i] = u[i] * inv
        base[i] = src[i] * inv

    def neighbours(v, i):
        flat = v.reshape(v.shape[0] * rows, lanes)
        here = v[i]
        below = flat[pl.ds(i * rows + unit, rows), :]
        cut = rows - 8
        below = jnp.concatenate([below[:cut], jnp.where(last_row, 0.0, below[cut:])], axis=0)
        right = jnp.where(last_lane, 0.0, pltpu.roll(here, lanes - 1, 1))
        total = even[i] * ((v[i + 1] + below) + right)
        total += low_z[i] * v[i - 1] + low_x[i] * flat[pl.ds(i * rows - unit, rows), :]
        return total + low_y[i] * pltpu.roll(here, 1, 1)

    powers, bases = [y0, y1, y2, y3], [u, v1, v2, v3]

    def lift(n, whole=True):
        def one(i):
            y = neighbours(powers[n - 1], i)
            b = base[i] + neighbours(bases[n - 1], i)
            if n < ITERS:
                powers[n][i] = y
                bases[n][i] = b
            else:
                g[i] = b
                e[i] = b + diagonal[i] * y
                if whole:
                    spread_sum(i)
        return one

    def raise_power(n):
        def one(i):
            powers[n][i] = neighbours(powers[n - 1], i)
        return one

    def raise_base(n):
        def one(i):
            bases[n][i] = base[i] + neighbours(bases[n - 1], i)
        return one

    def spread_sum(i):
        z[i] = (y0[i] + y1[i]) + (y2[i] + y3[i])

    def emit(k):
        swap(k).start()

        @pl.when(jnp.logical_and(odd == 1, k < early))
        def _():
            hand(k).start()

    loaded(0, 6 * half).wait()
    each(0, STEP + ITERS, coefficients)
    for n in range(1, ITERS):
        each(0, STEP + ITERS - n, raise_power(n))
    each(0, STEP, spread_sum)
    pl.semaphore_wait(barrier, greeted)

    @pl.when(odd == 1)
    def _():
        hand(0).start()

    for n in range(1, ITERS):
        each(0, STEP + ITERS - n, raise_base(n))
    each(0, STEP, lift(ITERS, False))
    swap(0).start()
    for copy in rims:
        copy.start()

    def local(k, carry):
        lo = STEP * k

        @pl.when(lo + ITERS == half)
        def _():
            loaded(1, 6 * (planes - half)).wait()

        @pl.when(lo + ITERS == planes)
        def _():
            total(1, 6 * HALO).wait_recv()

        pair(lo + ITERS, coefficients)
        for n in range(1, ITERS + 1):
            pair(lo + ITERS - n, lift(n))
        emit(k)
        return carry

    lax.fori_loop(1, count, local, 0)
    rim_g.start()

    def combine(k):
        @pl.when(odd == 0)
        def _():
            swap(k).wait_recv()

            def one(i):
                z[i] = z[i] + e_in[i]

            pair(STEP * k, one)
            hand(k).start()

    levels = [g, v1, v2, v3, s2]

    def force(i):
        forced[i] = (src[i] + r[i]) * inverse[i]

    def iterate(n):
        def one(i):
            levels[n][i] = forced[i] + neighbours(levels[n - 1], i)
        return one

    def gather(k):
        hand(k).wait_recv()

        @pl.when(odd == 1)
        def _():
            swap(k).wait_recv()

            def one(i):
                r[i] = z_in[i] + e_in[i]

            pair(STEP * k, one)

        @pl.when(odd == 0)
        def _():
            def one(i):
                r[i] = z_in[i]

            pair(STEP * k, one)

        pair(STEP * k, force)

    def act(order):
        for what in order:
            n = int(what[1:])
            if what[0] == "W":
                hand(n).start()
            else:
                slot = 1 if what[0] == "F" else 2
                arrival(slot, n).wait_recv()
                forward(slot, n).start()

    for k in range(LAG):
        combine(k)
    for k in range(LAG, 2 * LAG):
        @pl.when(time == 0)
        def _():
            combine(k)
    reached = [0] * (ITERS + 1)
    for k in range(2):
        combine(k + lag)
        gather(k)
        for n in range(1, ITERS + 1):
            goal = max(STEP * (k + 1) - (n - 1), 0)
            each(reached[n], goal, iterate(n))
            reached[n] = goal
    rim_g.wait_recv()

    def sweep(k, carry):
        @pl.when(k + lag < count)
        def _():
            combine(k + lag)

        gather(k)
        for n in range(1, ITERS + 1):
            pair(STEP * k - (n - 1), iterate(n))
        pass_on(k - 2).start()

        for where in range(len(ORDERS)):
            for turn in range(2, count):
                if ORDERS[where][turn - 2]:
                    @pl.when(jnp.logical_and(zone == where, k == turn))
                    def _():
                        act(ORDERS[where][turn - 2])

        return carry

    lax.fori_loop(2, count, sweep, 0)
    rim_r.start()
    rim_r.wait_recv()
    each(planes, planes + HALO - 1, force)
    for n in range(1, ITERS + 1):
        each(planes - (n - 1), planes + ITERS - n, iterate(n))
    rim_s.start()

    def close():
        pass_on(count - 2).start()
        pass_on(count - 1).start()

    @pl.when(zone != 1)
    def _():
        close()

    for where in range(len(ORDERS)):
        if ORDERS[where][-1]:
            @pl.when(zone == where)
            def _():
                act(ORDERS[where][-1])

    @pl.when(zone == 1)
    def _():
        close()

    rim_s.wait_recv()

    def partial(k, carry):
        def one(i):
            res[i] = src[i] - diagonal[i] * (s2[i] - neighbours(s2, i))

        pair(STEP * k, one)
        return carry

    lax.fori_loop(0, count, partial, 0)

    def settle(m, carry):
        arrival(0, m).wait_recv()

        def one(i):
            res[i] = res[i] + p3[i]

        pair(STEP * m, one)
        return carry

    lax.fori_loop(0, count, settle, 0)

    total(0, 3 * planes).wait_send()
    total(1, 8 * HALO).wait_send()
    for where, order in enumerate(ORDERS):
        passed = sum(what[0] != "W" for what in sum(order, []))
        if passed:
            @pl.when(zone == where)
            def _():
                total(2, STEP * passed).wait_send()


def finish(planes, s2, res, smoothed, residual, sem):
    size = planes // 2
    copies = []
    for lo in range(0, planes, size):
        copies.append(pltpu.make_async_copy(s2.at[pl.ds(HALO + lo, size)], smoothed.at[0, pl.ds(lo, size)], sem.at[0]))
        copies.append(pltpu.make_async_copy(res.at[pl.ds(HALO + lo, size)], residual.at[0, pl.ds(lo, size)], sem.at[1]))
    for copy in copies:
        copy.start()
    pltpu.make_async_copy(s2.at[pl.ds(HALO, planes)], smoothed.at[0], sem.at[0]).wait()
    pltpu.make_async_copy(res.at[pl.ds(HALO, planes)], residual.at[0], sem.at[1]).wait()


def body(steps, sides, initial, source, diffusion, advection):
    _, planes, rows, lanes = initial.shape
    assert sides == 2 and steps % 2 == 0 and planes % (2 * STEP) == 0
    count = planes // STEP
    shape = (planes + 2 * HALO, rows, lanes)
    wide = pltpu.VMEM(shape, jnp.float32)
    triple = pltpu.VMEM((3,) + shape, jnp.float32)
    slots = pltpu.VMEM((3 * shape[0],) + shape[1:], jnp.float32)
    dma = pltpu.SemaphoreType.DMA
    result = jax.ShapeDtypeStruct(initial.shape, jnp.float32)
    vmem = pl.BlockSpec(memory_space=pltpu.VMEM)
    hbm = pl.BlockSpec(memory_space=pltpu.HBM)
    grant = VMEM_BYTES - (2 * shape[0] + 4) * rows * lanes * 4
    held = pl.pallas_call(
        functools.partial(kernel, planes, steps),
        out_shape=(wide,) * 2,
        in_specs=[hbm] * 4,
        out_specs=(vmem,) * 2,
        scratch_shapes=[wide] * 3 + [triple] + [wide] * 21 + [slots]
        + [dma((2,)), dma((3,))] + [dma((count,))] * 2
        + [dma((count + 6,)), dma((4,))],
        compiler_params=pltpu.CompilerParams(collective_id=0, has_side_effects=True, vmem_limit_bytes=grant),
        name="smooth",
    )(initial, source, diffusion, advection)
    return pl.pallas_call(
        functools.partial(finish, planes),
        out_shape=(result, result),
        in_specs=[vmem] * 2,
        out_specs=(hbm,) * 2,
        scratch_shapes=[dma((2,))],
        compiler_params=pltpu.CompilerParams(vmem_limit_bytes=8 << 20),
        name="finish",
    )(*held)


def solution(mesh):
    in_specs = (
        P("tm", "space", None, None),
        P("tm", "space", None, None),
        P("space", None, None),
        P(None, "space", None, None),
    )
    out_specs = (P("tm", "space", None, None), P("tm", "space", None, None))
    run = functools.partial(body, mesh.shape["tm"], mesh.shape["space"])
    return jax.shard_map(run, mesh=mesh, in_specs=in_specs, out_specs=out_specs, check_vma=False)
```

```python
import functools

import jax
import jax.numpy as jnp
from jax import lax
from jax.experimental import pallas as pl
from jax.experimental.pallas import tpu as pltpu
from jax.sharding import PartitionSpec as P

ITERS = 4
HALO = ITERS
STEP = 2
LAG = 3
VMEM_BYTES = 67043328
MESH = pl.DeviceIdType.MESH
REACH = [3, 3, 3, 2, 0]
ROUND = ((2, 0), (2, 1), (1, 0), (1, 0), (1, 0), (0, 0), (0, 0), (0, 0))
EARLY = [5, 8, 5, 5, 8]
ORDERS = [
    [[], [], ["W5", "W6", "W7", "F0", "F1", "F2"], [], [], [], []],
    [[], [], [], [], [], [], ["F2", "F3", "F4"]],
    [[], [], ["W5", "W6", "W7"], [], ["F0"], ["F1"], ["F2"]],
    [[], [], ["W5", "W6", "W7", "F0", "F1", "F2"], [], [], [], []],
    [[], [], ["F0", "F1"], [], [], [], []],
    [[], [], [], ["G0"], [], [], []],
    [[], [], ["G1"], [], [], [], []],
]


def kernel(planes, steps, initial, source, diffusion, advection, s2, res,
           u, src, spread, upwind, low_z, low_x, low_y, even, inverse, diagonal,
           base, forced, y0, y1, y2, y3, v1, v2, v3, g, e, z, e_in, z_in, r, p3,
           load_sem, sent, recv_e, recv_z, recv_s, hrecv):
    count = planes // STEP
    half = STEP + ITERS
    time, side = lax.axis_index("tm"), lax.axis_index("space")
    odd = lax.rem(time, 2)
    partner = time + 1 - 2 * odd
    after, before = lax.rem(time + 1, steps), lax.rem(time + steps - 1, steps)
    beyond, behind = lax.rem(time + 2, steps), lax.rem(time + steps - 2, steps)
    other = 1 - side
    rows, lanes = u.shape[1], u.shape[2]

    def begin(lo, hi, who=side):
        return (1 - who) * (HALO + lo) + who * (HALO + planes - hi)

    def span(lo, hi, who=side):
        return pl.ds(begin(lo, hi, who), hi - lo if isinstance(lo, int) else STEP)

    def grid_span(lo, hi):
        return pl.ds(begin(lo, hi) - HALO, hi - lo)

    def part(k):
        return pl.ds(begin(STEP * k, STEP * k + STEP), STEP)

    zone = odd - 1 + sum(
        jnp.where(time == at, n, 0) for n, at in ((1, 1), (2, 3), (3, steps - 3), (4, steps - 1), (6, steps - 4), (7, steps - 2)))
    reach = sum(jnp.where(zone == n, REACH[n], 0) for n in range(len(REACH)))
    lag = LAG + jnp.where(time == 0, LAG, 0)
    early = sum(jnp.where(zone == n, EARLY[n], 0) for n in range(len(EARLY)))

    barrier = pltpu.get_barrier_semaphore()
    for peer in ((partner, side), (behind, side), (before, side), (time, other)):
        pl.semaphore_signal(barrier, inc=1, device_id=peer, device_id_type=MESH)
    guests = (steps - 4,)
    for guest in guests:
        for here, there in ((0, guest), (guest, steps - 1)):
            @pl.when(time == here)
            def _():
                pl.semaphore_signal(barrier, inc=1, device_id=(there, side), device_id_type=MESH)

    greeted = 4 + sum(jnp.where(zone == n, extra, 0) for n, extra in ((4, 1), (5, 1)))

    loads = []
    for n, (lo, hi) in enumerate(((0, half), (half, planes))):
        here, there = span(lo, hi), grid_span(lo, hi)
        loads.append([
            pltpu.make_async_copy(diffusion.at[there], spread.at[here], load_sem.at[n]),
            pltpu.make_async_copy(advection.at[:, there], upwind.at[:, here], load_sem.at[n]),
            pltpu.make_async_copy(initial.at[0, there], u.at[here], load_sem.at[n]),
            pltpu.make_async_copy(source.at[0, there], src.at[here], load_sem.at[n]),
        ])
    for group in loads:
        for load in group:
            load.start()

    edge = begin(-1, 0)
    for field in (u, y0, y1, y2, y3, v1, v2, v3, g, s2):
        field[edge] = jnp.zeros((rows, lanes), jnp.float32)

    def across(source_ref, target_ref, n):
        return pltpu.make_async_remote_copy(
            src_ref=source_ref, dst_ref=target_ref, send_sem=sent.at[1], recv_sem=hrecv.at[n],
            device_id=(time, other), device_id_type=MESH)

    def rim(field, width, n):
        return across(field.at[span(planes - width, planes)],
                      field.at[span(planes, planes + width, other)], n)

    mine, theirs = grid_span(planes - HALO, planes), span(planes, planes + HALO, other)
    rims = [
        across(diffusion.at[mine], spread.at[theirs], 0),
        across(advection.at[:, mine], upwind.at[:, theirs], 0),
        across(initial.at[0, mine], u.at[theirs], 0),
        across(source.at[0, mine], src.at[theirs], 0),
    ]
    rim_g, rim_r, rim_s = rim(g, HALO, 1), rim(r, HALO - 1, 2), rim(s2, 1, 3)

    def swap(k):
        return pltpu.make_async_remote_copy(
            src_ref=e.at[part(k)], dst_ref=e_in.at[part(k)], send_sem=sent.at[0], recv_sem=recv_e.at[k],
            device_id=(partner, side), device_id_type=MESH)

    def hand(k):
        return pltpu.make_async_remote_copy(
            src_ref=z.at[part(k)], dst_ref=z_in.at[part(k)], send_sem=sent.at[0], recv_sem=recv_z.at[k],
            device_id=(beyond, side), device_id_type=MESH)

    depth = planes + 2 * HALO

    def place(slot, m):
        return p3.at[pl.ds(slot * depth + begin(STEP * m, STEP * m + STEP), STEP)]

    def landed(slot, m):
        return recv_s.at[jnp.where(slot == 0, m, count + jnp.where(slot == 1, m % 4, 4 + m % 2))]

    def pass_on(m):
        near = jnp.where(m < reach, 1, 0)
        far = sum(jnp.where(m == n, slot, 0) for n, (slot, _) in enumerate(ROUND))
        slot = odd * jnp.where(zone == 4, far, near)
        host = sum(jnp.where(m == n, (steps - 4, steps - 2)[at], 0) for n, (slot_, at) in enumerate(ROUND) if slot_ == 2)
        to = jnp.where(slot == 0, after, jnp.where(slot == 1, beyond, host))
        return pltpu.make_async_remote_copy(
            src_ref=s2.at[part(m)], dst_ref=place(slot, m), send_sem=sent.at[0],
            recv_sem=landed(slot, m), device_id=(to, side), device_id_type=MESH)

    def forward(slot, m):
        to = before if slot == 1 else 0
        return pltpu.make_async_remote_copy(
            src_ref=place(slot, m), dst_ref=place(0, m), send_sem=sent.at[2],
            recv_sem=landed(0, m), device_id=(to, side), device_id_type=MESH)

    def arrival(slot, m):
        return pltpu.make_async_remote_copy(
            src_ref=s2.at[part(m)], dst_ref=place(slot, m), send_sem=sent.at[0],
            recv_sem=landed(slot, m), device_id=(after, side), device_id_type=MESH)

    def loaded(n, amount):
        return pltpu.make_async_copy(p3.at[pl.ds(0, amount)], p3.at[pl.ds(0, amount)], load_sem.at[n])

    def total(n, amount):
        return pltpu.make_async_remote_copy(
            src_ref=p3.at[pl.ds(0, amount)], dst_ref=p3.at[pl.ds(0, amount)], send_sem=sent.at[n],
            recv_sem=hrecv.at[0], device_id=(time, other), device_id_type=MESH)

    def each(lo, hi, body):
        start = begin(lo, hi)
        for k in range(hi - lo):
            body(start + k)

    def pair(lo, body):
        start = begin(lo, lo + STEP)
        for k in range(STEP):
            body(start + k)

    row = lax.broadcasted_iota(jnp.int32, (rows, lanes), 0)
    lane = lax.broadcasted_iota(jnp.int32, (rows, lanes), 1)
    last_row = lax.broadcasted_iota(jnp.int32, (8, lanes), 0) == 7
    last_lane = lane == lanes - 1
    unit = 1 + jnp.minimum(time, 0)

    def coefficients(i):
        d = spread[i]
        ax, ay, az = upwind[0, i], upwind[1, i], upwind[2, i]
        main = 1.0 + 6.0 * d + (ax + ay + az)
        inv = 1.0 / main
        even[i] = d * inv
        low_z[i] = (d + az) * inv
        low_x[i] = jnp.where(row == 0, 0.0, (d + ax) * inv)
        low_y[i] = jnp.where(lane == 0, 0.0, (d + ay) * inv)
        inverse[i] = inv
        diagonal[i] = main
        y0[i] = u[i] * inv
        base[i] = src[i] * inv

    def neighbours(v, i):
        flat = v.reshape(v.shape[0] * rows, lanes)
        here = v[i]
        below = flat[pl.ds(i * rows + unit, rows), :]
        cut = rows - 8
        below = jnp.concatenate([below[:cut], jnp.where(last_row, 0.0, below[cut:])], axis=0)
        right = jnp.where(last_lane, 0.0, pltpu.roll(here, lanes - 1, 1))
        total = even[i] * ((v[i + 1] + below) + right)
        total += low_z[i] * v[i - 1] + low_x[i] * flat[pl.ds(i * rows - unit, rows), :]
        return total + low_y[i] * pltpu.roll(here, 1, 1)

    powers, bases = [y0, y1, y2, y3], [u, v1, v2, v3]

    def lift(n, whole=True):
        def one(i):
            y = neighbours(powers[n - 1], i)
            b = base[i] + neighbours(bases[n - 1], i)
            if n < ITERS:
                powers[n][i] = y
                bases[n][i] = b
            else:
                g[i] = b
                e[i] = b + diagonal[i] * y
                if whole:
                    spread_sum(i)
        return one

    def raise_power(n):
        def one(i):
            powers[n][i] = neighbours(powers[n - 1], i)
        return one

    def raise_base(n):
        def one(i):
            bases[n][i] = base[i] + neighbours(bases[n - 1], i)
        return one

    def spread_sum(i):
        z[i] = (y0[i] + y1[i]) + (y2[i] + y3[i])

    def emit(k):
        swap(k).start()

        @pl.when(jnp.logical_and(odd == 1, k < early))
        def _():
            hand(k).start()

    loaded(0, 6 * half).wait()
    each(0, STEP + ITERS, coefficients)
    for n in range(1, ITERS):
        each(0, STEP + ITERS - n, raise_power(n))
    each(0, STEP, spread_sum)
    pl.semaphore_wait(barrier, greeted)

    @pl.when(odd == 1)
    def _():
        hand(0).start()

    for n in range(1, ITERS):
        each(0, STEP + ITERS - n, raise_base(n))
    each(0, STEP, lift(ITERS, False))
    swap(0).start()
    for copy in rims:
        copy.start()

    def local(k, carry):
        lo = STEP * k

        @pl.when(lo + ITERS == half)
        def _():
            loaded(1, 6 * (planes - half)).wait()

        @pl.when(lo + ITERS == planes)
        def _():
            total(1, 6 * HALO).wait_recv()

        pair(lo + ITERS, coefficients)
        for n in range(1, ITERS + 1):
            pair(lo + ITERS - n, lift(n))
        emit(k)
        return carry

    lax.fori_loop(1, count, local, 0)
    rim_g.start()

    def combine(k):
        @pl.when(odd == 0)
        def _():
            swap(k).wait_recv()

            def one(i):
                z[i] = z[i] + e_in[i]

            pair(STEP * k, one)
            hand(k).start()

    levels = [g, v1, v2, v3, s2]

    def force(i):
        forced[i] = (src[i] + r[i]) * inverse[i]

    def iterate(n):
        def one(i):
            levels[n][i] = forced[i] + neighbours(levels[n - 1], i)
        return one

    def gather(k):
        hand(k).wait_recv()

        @pl.when(odd == 1)
        def _():
            swap(k).wait_recv()

            def one(i):
                r[i] = z_in[i] + e_in[i]

            pair(STEP * k, one)

        @pl.when(odd == 0)
        def _():
            def one(i):
                r[i] = z_in[i]

            pair(STEP * k, one)

        pair(STEP * k, force)

    def act(order):
        for what in order:
            n = int(what[1:])
            if what[0] == "W":
                hand(n).start()
            else:
                slot = 1 if what[0] == "F" else 2
                arrival(slot, n).wait_recv()
                forward(slot, n).start()

    for k in range(LAG):
        combine(k)
    for k in range(LAG, 2 * LAG):
        @pl.when(time == 0)
        def _():
            combine(k)
    reached = [0] * (ITERS + 1)
    for k in range(2):
        combine(k + lag)
        gather(k)
        for n in range(1, ITERS + 1):
            goal = max(STEP * (k + 1) - (n - 1), 0)
            each(reached[n], goal, iterate(n))
            reached[n] = goal
    rim_g.wait_recv()

    def sweep(k, carry):
        @pl.when(k + lag < count)
        def _():
            combine(k + lag)

        gather(k)
        for n in range(1, ITERS + 1):
            pair(STEP * k - (n - 1), iterate(n))
        pass_on(k - 2).start()

        for where in range(len(ORDERS)):
            for turn in range(2, count):
                if ORDERS[where][turn - 2]:
                    @pl.when(jnp.logical_and(zone == where, k == turn))
                    def _():
                        act(ORDERS[where][turn - 2])

        return carry

    lax.fori_loop(2, count, sweep, 0)
    rim_r.start()
    rim_r.wait_recv()
    each(planes, planes + HALO - 1, force)
    for n in range(1, ITERS + 1):
        each(planes - (n - 1), planes + ITERS - n, iterate(n))
    rim_s.start()

    def close():
        pass_on(count - 2).start()
        pass_on(count - 1).start()

    @pl.when(zone != 1)
    def _():
        close()

    for where in range(len(ORDERS)):
        if ORDERS[where][-1]:
            @pl.when(zone == where)
            def _():
                act(ORDERS[where][-1])

    @pl.when(zone == 1)
    def _():
        close()

    rim_s.wait_recv()

    def partial(k, carry):
        def one(i):
            res[i] = src[i] - diagonal[i] * (s2[i] - neighbours(s2, i))

        pair(STEP * k, one)
        return carry

    lax.fori_loop(0, count, partial, 0)

    def settle(m, carry):
        arrival(0, m).wait_recv()

        def one(i):
            res[i] = res[i] + p3[i]

        pair(STEP * m, one)
        return carry

    lax.fori_loop(0, count, settle, 0)

    total(0, 3 * planes).wait_send()
    total(1, 8 * HALO).wait_send()
    for where, order in enumerate(ORDERS):
        passed = sum(what[0] != "W" for what in sum(order, []))
        if passed:
            @pl.when(zone == where)
            def _():
                total(2, STEP * passed).wait_send()


def finish(planes, s2, res, smoothed, residual, sem):
    size = planes // 2
    copies = []
    for lo in range(0, planes, size):
        copies.append(pltpu.make_async_copy(s2.at[pl.ds(HALO + lo, size)], smoothed.at[0, pl.ds(lo, size)], sem.at[0]))
        copies.append(pltpu.make_async_copy(res.at[pl.ds(HALO + lo, size)], residual.at[0, pl.ds(lo, size)], sem.at[1]))
    for copy in copies:
        copy.start()
    pltpu.make_async_copy(s2.at[pl.ds(HALO, planes)], smoothed.at[0], sem.at[0]).wait()
    pltpu.make_async_copy(res.at[pl.ds(HALO, planes)], residual.at[0], sem.at[1]).wait()


def body(steps, sides, initial, source, diffusion, advection):
    _, planes, rows, lanes = initial.shape
    assert sides == 2 and steps % 2 == 0 and steps >= 8 and planes % (2 * STEP) == 0
    count = planes // STEP
    shape = (planes + 2 * HALO, rows, lanes)
    wide = pltpu.VMEM(shape, jnp.float32)
    triple = pltpu.VMEM((3,) + shape, jnp.float32)
    slots = pltpu.VMEM((3 * shape[0],) + shape[1:], jnp.float32)
    dma = pltpu.SemaphoreType.DMA
    result = jax.ShapeDtypeStruct(initial.shape, jnp.float32)
    vmem = pl.BlockSpec(memory_space=pltpu.VMEM)
    hbm = pl.BlockSpec(memory_space=pltpu.HBM)
    grant = VMEM_BYTES - (2 * shape[0] + 4) * rows * lanes * 4
    held = pl.pallas_call(
        functools.partial(kernel, planes, steps),
        out_shape=(wide,) * 2,
        in_specs=[hbm] * 4,
        out_specs=(vmem,) * 2,
        scratch_shapes=[wide] * 3 + [triple] + [wide] * 21 + [slots]
        + [dma((2,)), dma((3,))] + [dma((count,))] * 2
        + [dma((count + 6,)), dma((4,))],
        compiler_params=pltpu.CompilerParams(collective_id=0, has_side_effects=True, vmem_limit_bytes=grant),
        name="smooth",
    )(initial, source, diffusion, advection)
    return pl.pallas_call(
        functools.partial(finish, planes),
        out_shape=(result, result),
        in_specs=[vmem] * 2,
        out_specs=(hbm,) * 2,
        scratch_shapes=[dma((2,))],
        compiler_params=pltpu.CompilerParams(vmem_limit_bytes=8 << 20),
        name="finish",
    )(*held)


def solution(mesh):
    in_specs = (
        P("tm", "space", None, None),
        P("tm", "space", None, None),
        P("space", None, None),
        P(None, "space", None, None),
    )
    out_specs = (P("tm", "space", None, None), P("tm", "space", None, None))
    run = functools.partial(body, mesh.shape["tm"], mesh.shape["space"])
    return jax.shard_map(run, mesh=mesh, in_specs=in_specs, out_specs=out_specs, check_vma=False)
```

```python
import functools

import jax
import jax.numpy as jnp
from jax import lax
from jax.experimental import pallas as pl
from jax.experimental.pallas import tpu as pltpu
from jax.sharding import PartitionSpec as P

ITERS = 4
HALO = ITERS
STEP = 2
LAG = 3
VMEM_BYTES = 67043328
MESH = pl.DeviceIdType.MESH
REACH = [3, 3, 3, 2, 0]
ROUND = ((2, 0), (2, 1), (1, 0), (1, 0), (1, 0), (0, 0), (0, 0), (0, 0))
EARLY = [5, 8, 5, 5, 8]
ORDERS = [
    [[], [], ["W5", "W6", "W7", "F0", "F1", "F2"], [], [], [], []],
    [[], [], [], [], [], [], ["F2", "F3", "F4"]],
    [[], [], ["W5", "W6", "W7"], [], ["F0"], ["F1"], ["F2"]],
    [[], [], ["W5", "W6", "W7", "F0", "F1", "F2"], [], [], [], []],
    [[], [], ["F0", "F1"], [], [], [], []],
    [[], [], [], ["G0"], [], [], []],
    [[], [], ["G1"], [], [], [], []],
]


def kernel(planes, steps, initial, source, diffusion, advection, s2, res,
           u, src, spread, upwind, low_z, low_x, low_y, even, inverse, diagonal,
           base, forced, y0, y1, y2, y3, v1, v2, v3, g, e, z, e_in, z_in, r, p3,
           load_sem, sent, recv_e, recv_z, recv_s, hrecv):
    count = planes // STEP
    half = STEP + ITERS
    time, side = lax.axis_index("tm"), lax.axis_index("space")
    odd = lax.rem(time, 2)
    partner = time + 1 - 2 * odd
    after, before = lax.rem(time + 1, steps), lax.rem(time + steps - 1, steps)
    beyond, behind = lax.rem(time + 2, steps), lax.rem(time + steps - 2, steps)
    other = 1 - side
    rows, lanes = u.shape[1], u.shape[2]

    def begin(lo, hi, who=side):
        return (1 - who) * (HALO + lo) + who * (HALO + planes - hi)

    def span(lo, hi, who=side):
        return pl.ds(begin(lo, hi, who), hi - lo if isinstance(lo, int) else STEP)

    def grid_span(lo, hi):
        return pl.ds(begin(lo, hi) - HALO, hi - lo)

    def part(k):
        return pl.ds(begin(STEP * k, STEP * k + STEP), STEP)

    zone = odd - 1 + sum(
        jnp.where(time == at, n, 0) for n, at in ((1, 1), (2, 3), (3, steps - 3), (4, steps - 1), (6, steps - 4), (7, steps - 2)))
    reach = sum(jnp.where(zone == n, REACH[n], 0) for n in range(len(REACH)))
    lag = LAG + jnp.where(time == 0, LAG, 0)
    early = sum(jnp.where(zone == n, EARLY[n], 0) for n in range(len(EARLY)))

    barrier = pltpu.get_barrier_semaphore()
    for peer in ((partner, side), (behind, side), (before, side), (time, other)):
        pl.semaphore_signal(barrier, inc=1, device_id=peer, device_id_type=MESH)
    guests = (steps - 4,)
    for guest in guests:
        for here, there in ((0, guest), (guest, steps - 1)):
            @pl.when(time == here)
            def _():
                pl.semaphore_signal(barrier, inc=1, device_id=(there, side), device_id_type=MESH)

    greeted = 4 + sum(jnp.where(zone == n, extra, 0) for n, extra in ((4, 1), (5, 1)))

    loads = []
    for n, (lo, hi) in enumerate(((0, half), (half, planes))):
        here, there = span(lo, hi), grid_span(lo, hi)
        loads.append([
            pltpu.make_async_copy(diffusion.at[there], spread.at[here], load_sem.at[n]),
            pltpu.make_async_copy(advection.at[:, there], upwind.at[:, here], load_sem.at[n]),
            pltpu.make_async_copy(initial.at[0, there], u.at[here], load_sem.at[n]),
            pltpu.make_async_copy(source.at[0, there], src.at[here], load_sem.at[n]),
        ])
    for group in loads:
        for load in group:
            load.start()

    edge = begin(-1, 0)
    for field in (u, y0, y1, y2, y3, v1, v2, v3, g, s2):
        field[edge] = jnp.zeros((rows, lanes), jnp.float32)

    def across(source_ref, target_ref, n):
        return pltpu.make_async_remote_copy(
            src_ref=source_ref, dst_ref=target_ref, send_sem=sent.at[1], recv_sem=hrecv.at[n],
            device_id=(time, other), device_id_type=MESH)

    def rim(field, width, n):
        return across(field.at[span(planes - width, planes)],
                      field.at[span(planes, planes + width, other)], n)

    mine, theirs = grid_span(planes - HALO, planes), span(planes, planes + HALO, other)
    rims = [
        across(diffusion.at[mine], spread.at[theirs], 0),
        across(advection.at[:, mine], upwind.at[:, theirs], 0),
        across(initial.at[0, mine], u.at[theirs], 0),
        across(source.at[0, mine], src.at[theirs], 0),
    ]
    rim_g, rim_r, rim_s = rim(g, HALO, 1), rim(r, HALO - 1, 2), rim(s2, 1, 3)

    def swap(k):
        return pltpu.make_async_remote_copy(
            src_ref=e.at[part(k)], dst_ref=e_in.at[part(k)], send_sem=sent.at[0], recv_sem=recv_e.at[k],
            device_id=(partner, side), device_id_type=MESH)

    def hand(k):
        return pltpu.make_async_remote_copy(
            src_ref=z.at[part(k)], dst_ref=z_in.at[part(k)], send_sem=sent.at[0], recv_sem=recv_z.at[k],
            device_id=(beyond, side), device_id_type=MESH)

    depth = planes + 2 * HALO

    def place(slot, m):
        return p3.at[pl.ds(slot * depth + begin(STEP * m, STEP * m + STEP), STEP)]

    def landed(slot, m):
        return recv_s.at[jnp.where(slot == 0, jnp.maximum(m - (count - 3), 0), 3 + jnp.where(slot == 1, m % 4, 4 + m % 2))]

    def pass_on(m):
        near = jnp.where(m < reach, 1, 0)
        far = sum(jnp.where(m == n, slot, 0) for n, (slot, _) in enumerate(ROUND))
        slot = odd * jnp.where(zone == 4, far, near)
        host = sum(jnp.where(m == n, (steps - 4, steps - 2)[at], 0) for n, (slot_, at) in enumerate(ROUND) if slot_ == 2)
        to = jnp.where(slot == 0, after, jnp.where(slot == 1, beyond, host))
        return pltpu.make_async_remote_copy(
            src_ref=s2.at[part(m)], dst_ref=place(slot, m), send_sem=sent.at[0],
            recv_sem=landed(slot, m), device_id=(to, side), device_id_type=MESH)

    def forward(slot, m):
        to = before if slot == 1 else 0
        return pltpu.make_async_remote_copy(
            src_ref=place(slot, m), dst_ref=place(0, m), send_sem=sent.at[2],
            recv_sem=landed(0, m), device_id=(to, side), device_id_type=MESH)

    def arrival(slot, m):
        return pltpu.make_async_remote_copy(
            src_ref=s2.at[part(m)], dst_ref=place(slot, m), send_sem=sent.at[0],
            recv_sem=landed(slot, m), device_id=(after, side), device_id_type=MESH)

    def loaded(n, amount):
        return pltpu.make_async_copy(p3.at[pl.ds(0, amount)], p3.at[pl.ds(0, amount)], load_sem.at[n])

    def total(n, amount):
        return pltpu.make_async_remote_copy(
            src_ref=p3.at[pl.ds(0, amount)], dst_ref=p3.at[pl.ds(0, amount)], send_sem=sent.at[n],
            recv_sem=hrecv.at[0], device_id=(time, other), device_id_type=MESH)

    def each(lo, hi, body):
        start = begin(lo, hi)
        for k in range(hi - lo):
            body(start + k)

    def pair(lo, body):
        start = begin(lo, lo + STEP)
        for k in range(STEP):
            body(start + k)

    row = lax.broadcasted_iota(jnp.int32, (rows, lanes), 0)
    lane = lax.broadcasted_iota(jnp.int32, (rows, lanes), 1)
    last_row = lax.broadcasted_iota(jnp.int32, (8, lanes), 0) == 7
    last_lane = lane == lanes - 1
    unit = 1 + jnp.minimum(time, 0)

    def coefficients(i):
        d = spread[i]
        ax, ay, az = upwind[0, i], upwind[1, i], upwind[2, i]
        main = 1.0 + 6.0 * d + (ax + ay + az)
        inv = 1.0 / main
        even[i] = d * inv
        low_z[i] = (d + az) * inv
        low_x[i] = jnp.where(row == 0, 0.0, (d + ax) * inv)
        low_y[i] = jnp.where(lane == 0, 0.0, (d + ay) * inv)
        inverse[i] = inv
        diagonal[i] = main
        y0[i] = u[i] * inv
        base[i] = src[i] * inv

    def neighbours(v, i):
        flat = v.reshape(v.shape[0] * rows, lanes)
        here = v[i]
        below = flat[pl.ds(i * rows + unit, rows), :]
        cut = rows - 8
        below = jnp.concatenate([below[:cut], jnp.where(last_row, 0.0, below[cut:])], axis=0)
        right = jnp.where(last_lane, 0.0, pltpu.roll(here, lanes - 1, 1))
        total = even[i] * ((v[i + 1] + below) + right)
        total += low_z[i] * v[i - 1] + low_x[i] * flat[pl.ds(i * rows - unit, rows), :]
        return total + low_y[i] * pltpu.roll(here, 1, 1)

    powers, bases = [y0, y1, y2, y3], [u, v1, v2, v3]

    def lift(n, whole=True):
        def one(i):
            y = neighbours(powers[n - 1], i)
            b = base[i] + neighbours(bases[n - 1], i)
            if n < ITERS:
                powers[n][i] = y
                bases[n][i] = b
            else:
                g[i] = b
                e[i] = b + diagonal[i] * y
                if whole:
                    spread_sum(i)
        return one

    def raise_power(n):
        def one(i):
            powers[n][i] = neighbours(powers[n - 1], i)
        return one

    def raise_base(n):
        def one(i):
            bases[n][i] = base[i] + neighbours(bases[n - 1], i)
        return one

    def spread_sum(i):
        z[i] = (y0[i] + y1[i]) + (y2[i] + y3[i])

    def emit(k):
        swap(k).start()

        @pl.when(jnp.logical_and(odd == 1, k < early))
        def _():
            hand(k).start()

    loaded(0, 6 * half).wait()
    each(0, STEP + ITERS, coefficients)
    for n in range(1, ITERS):
        each(0, STEP + ITERS - n, raise_power(n))
    each(0, STEP, spread_sum)
    pl.semaphore_wait(barrier, greeted)

    @pl.when(odd == 1)
    def _():
        hand(0).start()

    for n in range(1, ITERS):
        each(0, STEP + ITERS - n, raise_base(n))
    each(0, STEP, lift(ITERS, False))
    swap(0).start()
    for copy in rims:
        copy.start()

    def local(k, carry):
        lo = STEP * k

        @pl.when(lo + ITERS == half)
        def _():
            loaded(1, 6 * (planes - half)).wait()

        @pl.when(lo + ITERS == planes)
        def _():
            total(1, 6 * HALO).wait_recv()

        pair(lo + ITERS, coefficients)
        for n in range(1, ITERS + 1):
            pair(lo + ITERS - n, lift(n))
        emit(k)
        return carry

    lax.fori_loop(1, count, local, 0)
    rim_g.start()

    def combine(k):
        @pl.when(odd == 0)
        def _():
            swap(k).wait_recv()

            def one(i):
                z[i] = z[i] + e_in[i]

            pair(STEP * k, one)
            hand(k).start()

    levels = [g, v1, v2, v3, s2]

    def force(i):
        forced[i] = (src[i] + r[i]) * inverse[i]

    def iterate(n):
        def one(i):
            levels[n][i] = forced[i] + neighbours(levels[n - 1], i)
        return one

    def gather(k):
        hand(k).wait_recv()

        @pl.when(odd == 1)
        def _():
            swap(k).wait_recv()

            def one(i):
                r[i] = z_in[i] + e_in[i]

            pair(STEP * k, one)

        @pl.when(odd == 0)
        def _():
            def one(i):
                r[i] = z_in[i]

            pair(STEP * k, one)

        pair(STEP * k, force)

    def act(order):
        for what in order:
            n = int(what[1:])
            if what[0] == "W":
                hand(n).start()
            else:
                slot = 1 if what[0] == "F" else 2
                arrival(slot, n).wait_recv()
                forward(slot, n).start()

    for k in range(LAG):
        combine(k)
    for k in range(LAG, 2 * LAG):
        @pl.when(time == 0)
        def _():
            combine(k)
    reached = [0] * (ITERS + 1)
    for k in range(2):
        combine(k + lag)
        gather(k)
        for n in range(1, ITERS + 1):
            goal = max(STEP * (k + 1) - (n - 1), 0)
            each(reached[n], goal, iterate(n))
            reached[n] = goal
    rim_g.wait_recv()

    def sweep(k, carry):
        @pl.when(k + lag < count)
        def _():
            combine(k + lag)

        gather(k)
        for n in range(1, ITERS + 1):
            pair(STEP * k - (n - 1), iterate(n))
        pass_on(k - 2).start()

        for where in range(len(ORDERS)):
            for turn in range(2, count):
                if ORDERS[where][turn - 2]:
                    @pl.when(jnp.logical_and(zone == where, k == turn))
                    def _():
                        act(ORDERS[where][turn - 2])

        return carry

    lax.fori_loop(2, count, sweep, 0)
    rim_r.start()
    rim_r.wait_recv()
    each(planes, planes + HALO - 1, force)
    for n in range(1, ITERS + 1):
        each(planes - (n - 1), planes + ITERS - n, iterate(n))
    rim_s.start()

    def close():
        pass_on(count - 2).start()
        pass_on(count - 1).start()

    @pl.when(zone != 1)
    def _():
        close()

    for where in range(len(ORDERS)):
        if ORDERS[where][-1]:
            @pl.when(zone == where)
            def _():
                act(ORDERS[where][-1])

    @pl.when(zone == 1)
    def _():
        close()

    rim_s.wait_recv()

    def partial(k, carry):
        def one(i):
            res[i] = src[i] - diagonal[i] * (s2[i] - neighbours(s2, i))

        pair(STEP * k, one)
        return carry

    lax.fori_loop(0, count, partial, 0)

    bulk = STEP * (count - 2)
    pltpu.make_async_remote_copy(
        src_ref=p3.at[pl.ds(0, bulk)], dst_ref=p3.at[pl.ds(0, bulk)], send_sem=sent.at[0],
        recv_sem=recv_s.at[0], device_id=(after, side), device_id_type=MESH).wait_recv()

    def settle(m, carry):
        @pl.when(m >= count - 2)
        def _():
            arrival(0, m).wait_recv()

        def one(i):
            res[i] = res[i] + p3[i]

        pair(STEP * m, one)
        return carry

    lax.fori_loop(0, count, settle, 0)

    total(0, 3 * planes).wait_send()
    total(1, 8 * HALO).wait_send()
    for where, order in enumerate(ORDERS):
        passed = sum(what[0] != "W" for what in sum(order, []))
        if passed:
            @pl.when(zone == where)
            def _():
                total(2, STEP * passed).wait_send()


def finish(planes, s2, res, smoothed, residual, sem):
    size = planes // 2
    copies = []
    for lo in range(0, planes, size):
        copies.append(pltpu.make_async_copy(s2.at[pl.ds(HALO + lo, size)], smoothed.at[0, pl.ds(lo, size)], sem.at[0]))
        copies.append(pltpu.make_async_copy(res.at[pl.ds(HALO + lo, size)], residual.at[0, pl.ds(lo, size)], sem.at[1]))
    for copy in copies:
        copy.start()
    pltpu.make_async_copy(s2.at[pl.ds(HALO, planes)], smoothed.at[0], sem.at[0]).wait()
    pltpu.make_async_copy(res.at[pl.ds(HALO, planes)], residual.at[0], sem.at[1]).wait()


def body(steps, sides, initial, source, diffusion, advection):
    _, planes, rows, lanes = initial.shape
    assert sides == 2 and steps % 2 == 0 and steps >= 8 and planes % (2 * STEP) == 0
    count = planes // STEP
    shape = (planes + 2 * HALO, rows, lanes)
    wide = pltpu.VMEM(shape, jnp.float32)
    triple = pltpu.VMEM((3,) + shape, jnp.float32)
    slots = pltpu.VMEM((3 * shape[0],) + shape[1:], jnp.float32)
    dma = pltpu.SemaphoreType.DMA
    result = jax.ShapeDtypeStruct(initial.shape, jnp.float32)
    vmem = pl.BlockSpec(memory_space=pltpu.VMEM)
    hbm = pl.BlockSpec(memory_space=pltpu.HBM)
    grant = VMEM_BYTES - (2 * shape[0] + 4) * rows * lanes * 4
    held = pl.pallas_call(
        functools.partial(kernel, planes, steps),
        out_shape=(wide,) * 2,
        in_specs=[hbm] * 4,
        out_specs=(vmem,) * 2,
        scratch_shapes=[wide] * 3 + [triple] + [wide] * 21 + [slots]
        + [dma((2,)), dma((3,))] + [dma((count,))] * 2
        + [dma((9,)), dma((4,))],
        compiler_params=pltpu.CompilerParams(collective_id=0, has_side_effects=True, vmem_limit_bytes=grant),
        name="smooth",
    )(initial, source, diffusion, advection)
    return pl.pallas_call(
        functools.partial(finish, planes),
        out_shape=(result, result),
        in_specs=[vmem] * 2,
        out_specs=(hbm,) * 2,
        scratch_shapes=[dma((2,))],
        compiler_params=pltpu.CompilerParams(vmem_limit_bytes=8 << 20),
        name="finish",
    )(*held)


def solution(mesh):
    in_specs = (
        P("tm", "space", None, None),
        P("tm", "space", None, None),
        P("space", None, None),
        P(None, "space", None, None),
    )
    out_specs = (P("tm", "space", None, None), P("tm", "space", None, None))
    run = functools.partial(body, mesh.shape["tm"], mesh.shape["space"])
    return jax.shard_map(run, mesh=mesh, in_specs=in_specs, out_specs=out_specs, check_vma=False)
```
